256 devices in a mesh: clips: 2 (over z), rows: 128 (over x, y, core).
Axes of the slice: x: 8, y: 8, z: 2, core: 2. Of those that a mesh axis runs over, the one named last changes fastest.
The devices are a block of a 8x8x16 slice.
Arguments:
- tokens: bfloat16 [1024, 120, 2240], P(('clips', 'rows')), parts along dimension 0, may hold values from -16 to 16
- shift: float32 [4480], P('clips'), parts along dimension 0, may hold values from -5 to 5
- scale: float32 [4480], P('clips'), parts along dimension 0, may hold values from -3 to 3
- gate: float32 [4480], P('clips'), parts along dimension 0, may hold values from -5 to 5
- query_weight: bfloat16 [2240, 1280], P(None, 'rows'), may hold values from -0.125 to 0.125
- pair_weight: bfloat16 [2240, 2560], P(None, 'rows'), may hold values from -0.125 to 0.125
- output_weight: bfloat16 [1280, 2240], P('rows'), may hold values from -0.15625 to 0.15625
- depth_taps: float32 [9, 1280], replicated, may hold values from -2 to 2
Outputs:
- block_out: bfloat16 [1024, 120, 2240], P(('clips', 'rows')), parts along dimension 0
- kv_state: float32 [80, 32, 32], P('clips'), parts along dimension 0
The draws below stay inside these ranges and needn't reach their ends.
There are 2 independent parts, one for each index of `clips`. The reference program is written for one: setup_inputs(seed, part) draws one part's arguments, and reference() takes and returns one part's arrays. A program takes and returns all parts, laid end to end along the dimension named above; an argument that names none is the same for every part. Nothing has to cross between parts.
All inputs are finite; a program needn't handle non-finite values.
Results may differ from the reference program's by a relative error of at most 0.0041.
The reference program's roundings to bfloat16 on the way (of `normed`, `query`, `keys`, `values` and `mixed`) count: a program that leaves them out, or rounds other values in their place, can miss the bound.
Values may be sent and summed in bfloat16 or wider, within the bound.
A program may use at most 128 MiB of HBM per device.

```python
import jax
import jax.numpy as jnp
from jax import lax

D = 2240
HEADS = 40
HEAD = 32
FRAMES = 8
COLS = 120
BAND = 4
HD = 1280
NR = 512
HEIGHT = 64
N_ROWS = 128


def draw_tokens(key, part):
    subkeys = jax.random.split(jax.random.fold_in(key, 7141), 4)
    row_index = jnp.arange(NR, dtype=jnp.int32)
    band_index = row_index // BAND
    frame_row = band_index // FRAMES * BAND + row_index % BAND
    frame_index = band_index % FRAMES
    row_ramp = 2.0 * frame_row.astype(jnp.float32) / max(HEIGHT - 1, 1) - 1.0
    frame_tilt = 2.0 * frame_index.astype(jnp.float32) / max(FRAMES - 1, 1) - 1.0
    row_direction = jax.random.normal(subkeys[0], (D,), jnp.float32)
    frame_direction = jax.random.normal(subkeys[1], (D,), jnp.float32)
    base_noise = jax.random.normal(subkeys[2], (NR, COLS, D), jnp.float32)
    strength = 1.5
    band_count = NR // BAND
    block_width = max(D // band_count, 1)
    pairing = jax.random.permutation(subkeys[3], band_count)
    feature_block = jnp.arange(D, dtype=jnp.int32) // block_width
    spiked = (feature_block[None, :] == pairing[band_index][:, None]).astype(jnp.float32)
    factor = 1.0 + 3.0 * spiked
    offset = strength * (row_ramp[:, None, None] * row_direction[None, None, :] + 0.5 * frame_tilt[:, None, None] * frame_direction[None, None, :])
    result = base_noise * factor[:, None, :] + offset
    return jnp.clip(result, -16.0, 16.0).astype(jnp.bfloat16)


def level_of(key, extent, pieces, smallest, top_value):
    factor_of, own = 1.0, jax.random.fold_in(key, 6)
    for axis_at, parts in pieces:
        draws = jnp.exp(jax.random.uniform(jax.random.fold_in(own, axis_at), (parts,), jnp.float32, smallest / len(pieces), top_value / len(pieces)))
        factor_of = factor_of * jnp.repeat(draws, extent[axis_at] // parts).reshape([-1 if axis == axis_at else 1 for axis in range(len(extent))])
    return factor_of


def centred(key, extent, scale, limit, cuts=(), held_as=jnp.bfloat16):
    gain = level_of(key, extent, cuts, -0.22, 0.18) if cuts else 1.0
    drawn = jax.random.normal(key, extent, jnp.float32) * scale * gain
    return jnp.minimum(jnp.maximum(drawn, -limit), limit).astype(held_as)


def setup_inputs(seed: int = 0, part: int = 0) -> dict:
    arg_keys = jax.random.split(jax.random.key(seed), 9)
    part_keys = jax.random.split(jax.random.fold_in(arg_keys[8], part), 9)
    return {
        "tokens": draw_tokens(jax.random.fold_in(jax.random.fold_in(arg_keys[8], part), 71), part),
        "shift": centred(part_keys[1], (D,), 1.0, 5.0, (), jnp.float32),
        "scale": centred(part_keys[2], (D,), 0.5, 3.0, (), jnp.float32),
        "gate": centred(part_keys[3], (D,), 1.0, 5.0, (), jnp.float32),
        "query_weight": centred(arg_keys[4], (D, HD), D ** -0.5, 0.125, ((1, 128),)),
        "pair_weight": centred(arg_keys[5], (D, 2 * HD), D ** -0.5, 0.125, ((1, 128),)),
        "output_weight": centred(arg_keys[6], (HD, D), HD ** -0.5, 0.15625, ((0, 128),)),
        "depth_taps": centred(arg_keys[7], (9, HD), 0.3, 2.0, (), jnp.float32),
    }


NORM_EPS = 1e-06
DENOM_EPS = 1e-06

def modulate(tokens, shift, scale):
    values = tokens.astype(jnp.float32)
    center = values - lax.optimization_barrier(jnp.mean(values, axis=-1, keepdims=True))
    spread = lax.optimization_barrier(jnp.mean(center * center, axis=-1, keepdims=True))
    return (center * lax.rsqrt(spread + NORM_EPS) * (1.0 + scale) + shift).astype(jnp.bfloat16)

def frame_conv(values, depth_taps):
    height, width = (values.shape[0], values.shape[1])
    padded = jnp.pad(values, ((1, 1), (1, 1), (0, 0)))
    result = jnp.zeros(values.shape, jnp.float32)
    for step_row in range(3):
        for step_col in range(3):
            taken = padded[step_row:step_row + height, step_col:step_col + width]
            result = result + depth_taps[3 * step_row + step_col] * taken
    return result

def reference(tokens, shift, scale, gate, query_weight, pair_weight, output_weight, depth_taps):
    bands_per_frame = N_ROWS // FRAMES
    band = NR // N_ROWS
    frames_grid = tokens.reshape(bands_per_frame, FRAMES, band, COLS, D).transpose(1, 0, 2, 3, 4).reshape(FRAMES, HEIGHT, COLS, D)

    def project(frame):
        normed = modulate(frame, shift, scale).reshape(HEIGHT * COLS, D)
        query = jnp.maximum(jnp.dot(normed, query_weight, preferred_element_type=jnp.float32), 0.0).astype(jnp.bfloat16)
        pair = jnp.dot(normed, pair_weight, preferred_element_type=jnp.float32)
        keys = jnp.maximum(pair[:, :HD], 0.0).astype(jnp.bfloat16)
        values = pair[:, HD:].astype(jnp.bfloat16)
        key_heads = keys.astype(jnp.float32).reshape(-1, HEADS, HEAD)
        value_heads = values.astype(jnp.float32).reshape(-1, HEADS, HEAD)
        state = jnp.einsum('thd,the->hde', key_heads, value_heads)
        return (query, values, state, lax.optimization_barrier(jnp.sum(key_heads, axis=0)))
    query, values, states, key_sums = lax.map(project, frames_grid)
    state = lax.optimization_barrier(jnp.sum(states, axis=0))
    key_sum = lax.optimization_barrier(jnp.sum(key_sums, axis=0))
    kv_state = state / (NR * COLS)

    def attend(inputs):
        frame, frame_query, frame_values = inputs
        local = frame_conv(frame_values.reshape(HEIGHT, COLS, HD), depth_taps).reshape(HEIGHT * COLS, HD)
        query_heads = frame_query.astype(jnp.float32).reshape(-1, HEADS, HEAD)
        numerator = jnp.einsum('thd,hde->the', query_heads, state, precision=lax.Precision.HIGHEST)
        denominator = jnp.einsum('thd,hd->th', query_heads, key_sum, precision=lax.Precision.HIGHEST) + DENOM_EPS
        linear = (numerator / denominator[:, :, None]).reshape(-1, HD)
        mixed = (linear + local).astype(jnp.bfloat16)
        projected = jnp.dot(mixed, output_weight, preferred_element_type=jnp.float32)
        result = frame.reshape(-1, D).astype(jnp.float32) + gate * projected
        return result.astype(jnp.bfloat16).reshape(HEIGHT, COLS, D)
    result = lax.map(attend, (frames_grid, query, values))
    block_out = result.reshape(FRAMES, bands_per_frame, band, COLS, D).transpose(1, 0, 2, 3, 4).reshape(NR, COLS, D)
    return (block_out, kv_state)
```

```python
import jax
import jax.numpy as jnp
from jax import lax
from jax.experimental import pallas as pl
from jax.experimental.pallas import tpu as pltpu
from jax.sharding import PartitionSpec as P

HEADS, HEAD, FRAMES, HD = 40, 32, 8, 1280
NORM_EPS = 1e-06
DENOM_EPS = 1e-06
SIDE = 8
UNIT = 80
D = 2240
KP = 2304
WA, WB = 640, 512
BASE1 = 2 * WA
F32, BF16 = jnp.float32, jnp.bfloat16
NT = (((1,), (1,)), ((), ()))
TN = (((0,), (0,)), ((), ()))
NN = (((1,), (0,)), ((), ()))


def mm(lhs, rhs, dims):
    return lax.dot_general(lhs, rhs, dims, preferred_element_type=F32)


def rem(v, m):
    return lax.rem(v + m, m)


def gather_parts(kvsh, qsh, osh, W0, W1, st_kv, st_qo, tmp, p0s, p0r, q0s, q0r, r1s, r1r, r2s, r2r, sbs, sbr):
    r = lax.axis_index("rows")
    c = lax.rem(r, 2)
    y = lax.rem(r // 2, SIDE)
    x = r // (2 * SIDE)
    j, p = y // 2, lax.rem(y, 2)
    i4 = y // 4
    t_me = lax.rem(y // 2, 2)
    a = jnp.where(c == 0, y, x)
    b = jnp.where(c == 0, x, y)
    wid = {0: WA, 1: WB}

    def dev(xx, yy, cc):
        return {"rows": (xx * SIDE + yy) * 2 + cc}

    def at_ring(aa, bb):
        xx = jnp.where(c == 0, bb, aa)
        yy = jnp.where(c == 0, aa, bb)
        return dev(xx, yy, c)

    def by_core(fn):
        for cc in (0, 1):
            @pl.when(c == cc)
            def _(cc=cc):
                fn(cc)

    def coff(cc, pp):
        return pl.multiple_of(pp * WA, 128) if cc == 0 else pl.multiple_of(BASE1 + pp * WB, 128)

    def piece(cc, s, aa, bb):
        xx, yy = (bb, aa) if cc == 0 else (aa, bb)
        cols = pl.ds(coff(cc, lax.rem(yy, 2)), wid[cc])
        if s == 0:
            return W0.at[xx, yy // 2, :, cols]
        return W1.at[lax.rem(yy // 2, 2), xx, yy // 4, :, cols]

    def barrier():
        sem = pltpu.get_barrier_semaphore()
        n = 0
        for m in range(1, 8):
            q = lax.rem(lax.rem(y, 4) * 2 + c + m, 8)
            pl.semaphore_signal(sem, inc=1, device_id=dev(x, 4 * i4 + q // 2, lax.rem(q, 2)))
            pl.semaphore_signal(sem, inc=1, device_id=dev(rem(x + m, SIDE), y, c))
            pl.semaphore_signal(sem, inc=1, device_id=dev(x, rem(y + m, SIDE), c))
            n += 3
        total = 2 * SIDE * SIDE
        for step in (SIDE, total - SIDE):
            pl.semaphore_signal(sem, inc=1, device_id={"rows": lax.rem(r + step, total)})
            n += 1
        pl.semaphore_wait(sem, n)

    def rcopy(src, dst, ss, rs, d):
        return pltpu.make_async_remote_copy(src_ref=src, dst_ref=dst, send_sem=ss, recv_sem=rs, device_id=d,
                                            device_id_type=pl.DeviceIdType.MESH)

    def kv0(m):
        pd, cd = m // 2, m % 2
        src = kvsh.at[:, pl.ds(cd * BASE1 + pd * wid[cd], wid[cd])]
        slot = 2 * p + c
        dst = st_kv.at[slot, :, pl.ds(0, wid[cd])]
        return src, dst, slot, dev(x, 2 * j + pd, cd), (2 * p + c) == m

    def qo0(m):
        yd, cd = m // 2, m % 2
        pd, td = yd % 2, yd // 2
        sh = qsh if td == 0 else osh
        src = sh.at[:, pl.ds(cd * BASE1 + pd * wid[cd], wid[cd])]
        slot = lax.rem(y, 4) * 2 + c
        dst = st_qo.at[slot, :, pl.ds(0, wid[cd])]
        return src, dst, slot, dev(x, 4 * i4 + yd, cd), slot == m

    def phase0_start(n, what, ss, rs):
        for m in range(n):
            src, dst, slot, d, own = what(m)

            @pl.when(own)
            def _():
                pltpu.make_async_copy(src, dst, rs.at[m]).start()

            @pl.when(jnp.logical_not(own))
            def _():
                rcopy(src, dst, ss.at[m], rs.at[slot], d).start()

    def phase0_wait(n, what, stage, ss, rs):
        for m in range(n):
            def w(cc):
                ref = stage.at[m, :, pl.ds(0, wid[cc])]
                pltpu.make_async_copy(ref, ref, rs.at[m]).wait()
            by_core(w)

    def phase0_drain(n, what, ss, rs):
        for m in range(n):
            src, dst, slot, d, own = what(m)

            @pl.when(jnp.logical_not(own))
            def _():
                rcopy(src, dst, ss.at[m], rs.at[slot], d).wait_send()

    def build(s, n, stage):
        rows = UNIT // n
        for m in range(n):
            tmp[m * rows:(m + 1) * rows, :] = stage[m].astype(jnp.float32)

        def put(cc):
            piece(cc, s, a, b)[...] = tmp[:, :wid[cc]].astype(jnp.bfloat16)
        by_core(put)

    def ap(e):
        d = (e + 1) // 2
        return rem(a + jnp.where(lax.rem(e, 2) == 1, -d, d), SIDE), d

    def ring1(s, e, wait_only=False):
        aa, d = ap(e)
        odd = lax.rem(e, 2) == 1

        def cp(cc, dr, aa_):
            ref = piece(cc, s, aa_, b)
            return rcopy(ref, ref, r1s.at[s, dr, aa_], r1r.at[s, aa_], at_ring(rem(a + (1 if dr == 0 else SIDE - 1), SIDE), b))

        @pl.when(e > 0)
        def _():
            by_core(lambda cc: cp(cc, 0, aa).wait_recv())
        right = jnp.logical_or(e == 0, jnp.logical_and(odd, d < 4))
        left = jnp.logical_or(e == 0, jnp.logical_and(jnp.logical_not(odd), d < 3))

        @pl.when(right)
        def _():
            by_core(lambda cc: cp(cc, 0, aa).start())

        @pl.when(left)
        def _():
            by_core(lambda cc: cp(cc, 1, aa).start())

    def ring1_drain(s):
        @pl.loop(0, 8)
        def _(e):
            aa, d = ap(e)
            odd = lax.rem(e, 2) == 1

            def cp(cc, dr):
                ref = piece(cc, s, aa, b)
                return rcopy(ref, ref, r1s.at[s, dr, aa], r1r.at[s, aa], at_ring(rem(a + 1, SIDE), b))

            @pl.when(jnp.logical_or(e == 0, jnp.logical_and(odd, d < 4)))
            def _():
                by_core(lambda cc: cp(cc, 0).wait_send())

            @pl.when(jnp.logical_or(e == 0, jnp.logical_and(jnp.logical_not(odd), d < 3)))
            def _():
                by_core(lambda cc: cp(cc, 1).wait_send())

    def cp2(cc, s, dr, bb, aa, dl, e):
        ref = piece(cc, s, aa, bb)
        return rcopy(ref, ref, r2s.at[s, dr, dl, e], r2r.at[s, bb, aa], at_ring(a, rem(b + (1 if dr == 0 else SIDE - 1), SIDE)))

    def ring2(s, dl, e, wait):
        aa, _ = ap(e)
        for dr in (0, 1):
            bb = rem(b + (-dl if dr == 0 else dl), SIDE)
            if wait:
                by_core(lambda cc: cp2(cc, s, dr, bb, aa, dl, e).wait_recv())
            go = jnp.logical_or(dl < 3, (e < 4) if dr == 0 else (e >= 4))

            @pl.when(go)
            def _():
                by_core(lambda cc: cp2(cc, s, dr, bb, aa, dl, e).start())

    def ring2_last(s, e):
        aa, _ = ap(e)
        bb = rem(b + 4, SIDE)
        by_core(lambda cc: cp2(cc, s, 0, bb, aa, 3, e).wait_recv())

    def ring2_drain(s):
        @pl.loop(0, 32)
        def _(t):
            dl, e = t // 8, lax.rem(t, 8)
            aa, _ = ap(e)
            for dr in (0, 1):
                go = jnp.logical_or(dl < 3, (e < 4) if dr == 0 else (e >= 4))

                @pl.when(go)
                def _():
                    by_core(lambda cc: cp2(cc, s, dr, b, aa, dl, e).wait_send())

    def sib_ref(cc, s, bb):
        if cc == 0:
            cols = pl.ds(0, 2 * WA)
            return W0.at[bb, :, :, cols] if s == 0 else W1.at[:, bb, :, :, cols]
        cols = pl.ds(coff(1, lax.rem(bb, 2)), WB)
        if s == 0:
            return W0.at[:, bb // 2, :, cols]
        return W1.at[lax.rem(bb // 2, 2), :, bb // 4, :, cols]

    def sib(cc, s, bb):
        ref = sib_ref(cc, s, bb)
        return rcopy(ref, ref, sbs.at[s, bb], sbr.at[s, bb], dev(x, y, 1 - c))

    def sib_start(s, bb):
        by_core(lambda cc: sib(cc, s, bb).start())

    def sib_wait(s):
        @pl.loop(0, SIDE)
        def _(bb):
            by_core(lambda cc: sib(1 - cc, s, bb).wait_recv())

    def sib_drain(s):
        @pl.loop(0, SIDE)
        def _(bb):
            by_core(lambda cc: sib(cc, s, bb).wait_send())

    ns = dict(locals())
    return ns


def drain(S):
    S.phase0_drain(4, S.kv0, S.p0s, S.p0r)
    S.phase0_drain(8, S.qo0, S.q0s, S.q0r)
    for s in (0, 1):
        S.ring1_drain(s)
        S.ring2_drain(s)
        S.sib_drain(s)


class Parts:
    pass


def kernel(tok, shift, scale, gate, taps, kvsh, qsh, osh, out, kvs,
           W0, W1, st_kv, st_qo, tmp, p0s, p0r, q0s, q0r, r1s, r1r, r2s, r2r, sbs, sbr,
           normed, keys, vals, vpad, local, mixed, hsend, hrecv, pay, ara, red, rsx, part, agy, tot, fin,
           hs, hr, aas, aar, xs, xr, ys, yr, zs, zr, es, er):
    S = Parts()
    S.__dict__.update(gather_parts(kvsh, qsh, osh, W0, W1, st_kv, st_qo, tmp, p0s, p0r, q0s, q0r, r1s, r1r,
                                   r2s, r2r, sbs, sbr))
    r, x, y, c, b = S.r, S.x, S.y, S.c, S.b
    total = 2 * SIDE * SIDE
    n_tok, width, band = 480, 120, 4
    kv_w = W0.reshape(2 * HD, KP)
    q_w = W1.at[0].reshape(HD, KP)
    o_w = W1.at[1].reshape(HD, KP)

    def norm():
        normed[:, KP - 128:] = jnp.zeros((n_tok, 128), BF16)

        @pl.loop(0, n_tok // 16)
        def _(i):
            rows = pl.ds(pl.multiple_of(i * 16, 16), 16)
            v = tok[rows, :].astype(F32)
            center = v - jnp.mean(v, axis=-1, keepdims=True)
            spread = jnp.mean(center * center, axis=-1, keepdims=True)
            res = center * lax.rsqrt(spread + NORM_EPS) * (1.0 + scale[...]) + shift[...]
            normed[rows, 0:D] = res.astype(BF16)

    def lanes(i, n):
        return pl.ds(pl.multiple_of(i * n, n), n)

    def value_chunk(i):
        res = mm(normed[...], kv_w[pl.ds(pl.multiple_of(HD + i * 256, 256), 256), :], NT).astype(BF16)
        vals[:, lanes(i, 256)] = res
        wide = res.astype(F32)
        vpad[1:1 + band, :, lanes(i, 256)] = wide.reshape(band, width, 256)
        hsend[0, :, lanes(i, 256)] = wide[0:width].astype(BF16)
        hsend[1, :, lanes(i, 256)] = wide[n_tok - width:].astype(BF16)

    def key_chunk(i):
        res = mm(normed[...], kv_w[lanes(i, 256), :], NT)
        keys[:, lanes(i, 256)] = jnp.maximum(res, 0.0).astype(BF16)

    def q_chunk(i):
        res = mm(normed[...], q_w[lanes(i, 256), :], NT)
        keys[:, lanes(i, 256)] = jnp.maximum(res, 0.0).astype(BF16)

    def block_mask():
        i = lax.broadcasted_iota(jnp.int32, (128, 128), 0) // HEAD
        k = lax.broadcasted_iota(jnp.int32, (128, 128), 1) // HEAD
        return i == k

    def state_group(g):
        k = keys[:, lanes(g, 128)]
        s = mm(k, vals[:, lanes(g, 128)], TN)
        s = jnp.where(block_mask(), s, 0.0)
        s = s[0:32] + s[32:64] + s[64:96] + s[96:128]
        half, gg = g // 5, lax.rem(g, 5)
        pay[half, pl.ds(pl.multiple_of(gg * 32, 32), 32), :] = s
        ks = mm(jnp.ones((8, n_tok), BF16), k, NN)
        pay[half, pl.ds(160 + gg, 1), :] = ks[0:1]

    def halo(k):
        to = rem(r + (total - FRAMES if k == 0 else FRAMES), total)
        return S.rcopy(hsend.at[k], hrecv.at[k], hs.at[k], hr.at[k], {"rows": to})

    def sends(k):
        return r >= FRAMES if k == 0 else r < total - FRAMES

    def halo_start():
        for k in (0, 1):
            pl.when(sends(k))(lambda: halo(k).start())

    def halo_finish():
        for k in (0, 1):
            row = band + 1 if k == 0 else 0

            @pl.when(sends(1 - k))
            def _():
                halo(k).wait_recv()
                vpad[row] = hrecv[k].astype(F32)

            @pl.when(jnp.logical_not(sends(1 - k)))
            def _():
                vpad[row] = jnp.zeros((width, HD), F32)

    def conv_group(g):
        ln = lanes(g, 128)
        tp = taps[:, ln]
        col = lax.broadcasted_iota(jnp.int32, (width, 128), 0)
        acc = [None] * band
        for k in range(band + 2):
            v = vpad[k, :, ln]
            before = jnp.where(col == 0, 0.0, pltpu.roll(v, 1, 0))
            after = jnp.where(col == width - 1, 0.0, pltpu.roll(v, width - 1, 0))
            for o in range(band):
                m = k - o
                if 0 <= m <= 2:
                    term = tp[3 * m:3 * m + 1] * before + tp[3 * m + 1:3 * m + 2] * v + tp[3 * m + 2:3 * m + 3] * after
                    acc[o] = term if acc[o] is None else acc[o] + term
        for o in range(band):
            local[o * width:(o + 1) * width, ln] = acc[o]

    def arm():
        return S.rcopy(pay.at[1 - c], ara, aas, aar, S.dev(x, y, 1 - c))

    def ar_x(m):
        xx = rem(x + m, SIDE)
        return S.rcopy(red.at[xx], rsx.at[x], xs.at[xx], xr.at[x], S.dev(xx, y, c)), xx

    def ar_y(m):
        yy = rem(y + m, SIDE)
        return S.rcopy(part, agy.at[y], ys.at[yy], yr.at[y], S.dev(x, yy, c)), yy

    def ar_z(m):
        xx = rem(x + m, SIDE)
        return S.rcopy(tot, fin.at[c, x], zs.at[xx], zr.at[x], S.dev(xx, y, c)), xx

    def arrived(m, buf, sem, me):
        k = rem(me + m, SIDE)
        pltpu.make_async_copy(buf.at[k], buf.at[k], sem.at[k]).wait()

    def sum8(buf):
        acc = buf[0]
        for k in range(1, SIDE):
            acc = acc + buf[k]
        return acc

    def ar_a():
        arm().start()

    def ar_b():
        arm().wait_recv()
        mine = pay[c] + ara[...]
        for k in range(SIDE):
            red[k] = mine[24 * k:24 * k + 24]
        rsx[x] = red[x]
        for m in range(1, SIDE):
            ar_x(m)[0].start()

    def ar_c():
        for m in range(1, SIDE):
            arrived(m, rsx, xr, x)
        res = sum8(rsx)
        part[...] = res
        agy[y] = res
        for m in range(1, SIDE):
            ar_y(m)[0].start()

    def ar_d():
        for m in range(1, SIDE):
            arrived(m, agy, yr, y)
        res = sum8(agy)
        tot[...] = res
        fin[c, x] = res
        for m in range(1, SIDE):
            ar_z(m)[0].start()

    def fin_copy(h):
        return S.rcopy(fin.at[h], fin.at[h], es, er, S.dev(x, y, 1 - c))

    def ar_e():
        for m in range(1, SIDE):
            k = rem(x + m, SIDE)
            pltpu.make_async_copy(tot, tot, zr.at[k]).wait()
        fin_copy(c).start()

    def ar_drain():
        arm().wait_send()
        for m in range(1, SIDE):
            ar_x(m)[0].wait_send()
            ar_y(m)[0].wait_send()
            ar_z(m)[0].wait_send()
        fin_copy(c).wait_send()
        for k in (0, 1):
            pl.when(sends(k))(lambda: halo(k).wait_send())

    def state_of(g):
        half, gg = g // 5, g % 5
        rows = []
        for k in range(4):
            at = 32 * gg + 8 * k
            rows.append(fin[half, at // 24, at % 24:at % 24 + 8])
        return jnp.concatenate(rows, axis=0), fin[half, 6, 16 + gg:17 + gg]

    def linear_group(g):
        s, ks = state_of(g)
        for h in range(4):
            kvs[4 * g + h] = s[:, 32 * h:32 * h + 32] / float(n_tok * total)
        mask = block_mask()
        bd = jnp.where(mask, jnp.concatenate([s] * 4, axis=0), 0.0)
        kd = jnp.where(mask, jnp.transpose(jnp.broadcast_to(ks, (128, 128))), 0.0)
        rhs = jnp.concatenate([bd, kd], axis=1)
        hi = rhs.astype(BF16)
        rest = rhs - hi.astype(F32)
        mid = rest.astype(BF16)
        lo = (rest - mid.astype(F32)).astype(BF16)
        q = keys[:, 128 * g:128 * g + 128]
        res = mm(q, hi, NN) + mm(q, mid, NN) + mm(q, lo, NN)
        lin = res[:, 0:128] / (res[:, 128:256] + DENOM_EPS)
        mixed[:, 128 * g:128 * g + 128] = (lin + local[:, 128 * g:128 * g + 128]).astype(BF16)

    def out_chunk(cols, n):
        w = o_w[:, pl.ds(cols, 256)]
        res = mm(mixed[...], w, NN)
        if n < 256:
            res = res[:, :n]
        ln = pl.ds(cols, n)
        out[:, ln] = (tok[:, ln].astype(F32) + gate[:, ln] * res).astype(BF16)

    S.barrier()
    S.phase0_start(4, S.kv0, p0s, p0r)
    S.phase0_start(8, S.qo0, q0s, q0r)
    pay[0, 160:192, :] = jnp.zeros((32, 128), F32)
    pay[1, 160:192, :] = jnp.zeros((32, 128), F32)
    S.phase0_wait(4, S.kv0, st_kv, p0s, p0r)
    S.build(0, 4, st_kv)
    S.phase0_wait(8, S.qo0, st_qo, q0s, q0r)

    @pl.loop(0, 8)
    def _(e):
        S.ring1(0, e)
        S.ring2(0, 0, e, False)
    S.build(1, 8, st_qo)
    S.sib_start(0, b)
    norm()

    @pl.loop(0, 24)
    def _(t):
        dl, e = 1 + t // 8, lax.rem(t, 8)
        S.ring2(0, dl, e, True)

        @pl.when(dl == 1)
        def _():
            S.ring1(1, e)

        @pl.when(e == 7)
        def _():
            S.sib_start(0, rem(b - dl, SIDE))
            S.sib_start(0, rem(b + dl, SIDE))

    @pl.loop(0, 8)
    def _(e):
        S.ring2(1, 0, e, False)
        S.ring2_last(0, e)
    S.sib_start(0, rem(b + 4, SIDE))
    S.sib_start(1, b)
    S.sib_wait(0)

    @pl.loop(0, 24)
    def _(t):
        dl, e = 1 + t // 8, lax.rem(t, 8)
        S.ring2(1, dl, e, True)

        @pl.when(e == 7)
        def _():
            S.sib_start(1, rem(b - dl, SIDE))
            S.sib_start(1, rem(b + dl, SIDE))

        @pl.when(t < 5)
        def _():
            value_chunk(t)

        pl.when(t == 4)(halo_start)

        @pl.when(jnp.logical_and(t >= 5, t < 10))
        def _():
            key_chunk(t - 5)

        @pl.when(jnp.logical_and(t >= 10, t < 15))
        def _():
            state_group(2 * (t - 10))
            state_group(2 * (t - 10) + 1)

        pl.when(t == 14)(ar_a)
        pl.when(t == 15)(ar_b)
        pl.when(t == 17)(halo_finish)

        @pl.when(jnp.logical_and(t >= 17, t < 22))
        def _():
            conv_group(2 * (t - 17))
            conv_group(2 * (t - 17) + 1)

        pl.when(t == 19)(ar_c)
        pl.when(t == 22)(ar_d)

    @pl.loop(0, 8)
    def _(e):
        S.ring2_last(1, e)
    S.sib_start(1, rem(b + 4, SIDE))
    ar_e()
    S.sib_wait(1)

    @pl.loop(0, 5)
    def _(i):
        q_chunk(i)
    fin_copy(1 - c).wait_recv()
    for g in range(HD // 128):
        linear_group(g)

    @pl.loop(0, 8)
    def _(i):
        out_chunk(pl.multiple_of(i * 256, 256), 256)
    out_chunk(2048, 192)
    ar_drain()
    drain(S)


def body(tokens, shift, scale, gate, query_weight, pair_weight, output_weight, depth_taps):
    band, width, model = tokens.shape
    n = band * width
    pad = ((0, 0), (0, KP - model))
    dma = pltpu.SemaphoreType.DMA
    vm = pltpu.VMEM
    out, kvs = pl.pallas_call(
        kernel,
        out_shape=(jax.ShapeDtypeStruct((n, model), BF16), jax.ShapeDtypeStruct((HEADS, HEAD, HEAD), F32)),
        in_specs=[pl.BlockSpec(memory_space=vm)] * 8,
        out_specs=[pl.BlockSpec(memory_space=vm)] * 2,
        scratch_shapes=[
            vm((SIDE, 4, UNIT, KP), BF16), vm((2, SIDE, 2, UNIT, KP), BF16),
            vm((4, 20, WA), BF16), vm((8, 10, WA), BF16), vm((UNIT, WA), F32),
            dma((4,)), dma((4,)), dma((8,)), dma((8,)),
            dma((2, 2, 8)), dma((2, 8)), dma((2, 2, 4, 8)), dma((2, 8, 8)), dma((2, 8)), dma((2, 8)),
            vm((n, KP), BF16), vm((n, HD), BF16), vm((n, HD), BF16), vm((band + 2, width, HD), F32),
            vm((n, HD), F32), vm((n, HD), BF16), vm((2, width, HD), BF16), vm((2, width, HD), BF16),
            vm((2, 192, 128), F32), vm((192, 128), F32), vm((SIDE, 24, 128), F32), vm((SIDE, 24, 128), F32),
            vm((24, 128), F32), vm((SIDE, 24, 128), F32), vm((24, 128), F32), vm((2, SIDE, 24, 128), F32),
            dma((2,)), dma((2,)), dma, dma, dma((8,)), dma((8,)), dma((8,)), dma((8,)), dma((8,)), dma((8,)), dma, dma,
        ],
        compiler_params=pltpu.CompilerParams(collective_id=0, has_side_effects=True, vmem_limit_bytes=62 << 20),
    )(
        tokens.reshape(n, model), shift[None], scale[None], gate[None], depth_taps,
        jnp.pad(pair_weight.T, pad), jnp.pad(query_weight.T, pad), jnp.pad(output_weight, pad),
    )
    return out.reshape(band, width, model), kvs


def solution(mesh):
    in_specs = (
        P(("clips", "rows"), None, None),
        P("clips"),
        P("clips"),
        P("clips"),
        P(None, "rows"),
        P(None, "rows"),
        P("rows", None),
        P(),
    )
    out_specs = (P(("clips", "rows"), None, None), P("clips", None, None))
    return jax.shard_map(body, mesh=mesh, in_specs=in_specs, out_specs=out_specs, check_vma=False)
```

```python
import jax
import jax.numpy as jnp
from jax import lax
from jax.experimental import pallas as pl
from jax.experimental.pallas import tpu as pltpu
from jax.sharding import PartitionSpec as P

HEADS, HEAD, FRAMES, HD = 40, 32, 8, 1280
NORM_EPS = 1e-06
DENOM_EPS = 1e-06
SIDE = 8
UNIT = 80
D = 2240
KP = 2304
WIDTHS = ((640, 512), (896, 256))
WMAX = 896
F32, BF16 = jnp.float32, jnp.bfloat16
NT = (((1,), (1,)), ((), ()))
TN = (((0,), (0,)), ((), ()))
NN = (((1,), (0,)), ((), ()))


def mm(lhs, rhs, dims):
    return lax.dot_general(lhs, rhs, dims, preferred_element_type=F32)


def rem(v, m):
    return lax.rem(v + m, m)


def gather_parts(kvsh, qosh, W0, W1, st_kv, st_qo, tmp, p0s, p0r, q0s, q0r, r1s, r1r, r2s, r2r, sbs, sbr):
    r = lax.axis_index("rows")
    c = lax.rem(r, 2)
    y = lax.rem(r // 2, SIDE)
    x = r // (2 * SIDE)
    j, p = y // 2, lax.rem(y, 2)
    i4 = y // 4
    a = jnp.where(c == 0, y, x)
    b = jnp.where(c == 0, x, y)
    wid = WIDTHS

    def dev(xx, yy, cc):
        return {"rows": (xx * SIDE + yy) * 2 + cc}

    def at_ring(aa, bb):
        xx = jnp.where(c == 0, bb, aa)
        yy = jnp.where(c == 0, aa, bb)
        return dev(xx, yy, c)

    def by_core(fn):
        for cc in (0, 1):
            @pl.when(c == cc)
            def _(cc=cc):
                fn(cc)

    def coff(s, cc, pp):
        return pl.multiple_of(cc * 2 * wid[s][0] + pp * wid[s][cc], 128)

    def piece(cc, s, aa, bb):
        xx, yy = (bb, aa) if cc == 0 else (aa, bb)
        cols = pl.ds(coff(s, cc, lax.rem(yy, 2)), wid[s][cc])
        if s == 0:
            return W0.at[xx, yy // 2, :, cols]
        return W1.at[lax.rem(yy // 2 + xx, 2), xx // 2, lax.rem(xx, 2), yy // 4, :, cols]

    def barrier():
        sem = pltpu.get_barrier_semaphore()
        n = 0
        for m in range(1, 8):
            q = lax.rem(lax.rem(y, 4) * 2 + c + m, 8)
            pl.semaphore_signal(sem, inc=1, device_id=dev(x, 4 * i4 + q // 2, lax.rem(q, 2)))
            pl.semaphore_signal(sem, inc=1, device_id=dev(rem(x + m, SIDE), y, c))
            pl.semaphore_signal(sem, inc=1, device_id=dev(x, rem(y + m, SIDE), c))
            n += 3
        for k in (1, -1):
            pl.semaphore_signal(sem, inc=1, device_id=dev(rem(x + k, SIDE), rem(y + 2 * k, SIDE), c))
            n += 1
        pl.semaphore_wait(sem, n)

    def rcopy(src, dst, ss, rs, d):
        return pltpu.make_async_remote_copy(src_ref=src, dst_ref=dst, send_sem=ss, recv_sem=rs, device_id=d,
                                            device_id_type=pl.DeviceIdType.MESH)

    def kv0(m):
        pd, cd = m // 2, m % 2
        w = wid[0][cd]
        src = kvsh.at[:, pl.ds(cd * 2 * wid[0][0] + pd * w, w)]
        slot = 2 * p + c
        dst = st_kv.at[slot, :, pl.ds(0, w)]
        return src, dst, slot, dev(x, 2 * j + pd, cd), (2 * p + c) == m

    def qo0(m):
        yd, cd = m // 2, m % 2
        pd, td = yd % 2, lax.rem(yd // 2 + x, 2)
        w = wid[1][cd]
        src = qosh.at[td, :, pl.ds(cd * 2 * wid[1][0] + pd * w, w)]
        slot = lax.rem(y, 4) * 2 + c
        dst = st_qo.at[slot, :, pl.ds(0, w)]
        return src, dst, slot, dev(x, 4 * i4 + yd, cd), slot == m

    def phase0_start(n, what, ss, rs):
        for m in range(n):
            src, dst, slot, d, own = what(m)

            @pl.when(own)
            def _():
                pltpu.make_async_copy(src, dst, rs.at[m]).start()

            @pl.when(jnp.logical_not(own))
            def _():
                rcopy(src, dst, ss.at[m], rs.at[slot], d).start()

    def phase0_wait(n, s, stage, rs):
        for m in range(n):
            def w(cc):
                ref = stage.at[m, :, pl.ds(0, wid[s][cc])]
                pltpu.make_async_copy(ref, ref, rs.at[m]).wait()
            by_core(w)

    def phase0_drain(n, what, ss, rs):
        for m in range(n):
            src, dst, slot, d, own = what(m)

            @pl.when(jnp.logical_not(own))
            def _():
                rcopy(src, dst, ss.at[m], rs.at[slot], d).wait_send()

    def build(s, n, stage):
        rows = UNIT // n
        for m in range(n):
            tmp[m * rows:(m + 1) * rows, 0:stage.shape[-1]] = stage[m].astype(jnp.float32)

        def put(cc):
            piece(cc, s, a, b)[...] = tmp[:, :wid[s][cc]].astype(jnp.bfloat16)
        by_core(put)

    def ap(e):
        d = (e + 1) // 2
        return rem(a + jnp.where(lax.rem(e, 2) == 1, -d, d), SIDE), d

    def ring1(s, e, wait_only=False):
        aa, d = ap(e)
        odd = lax.rem(e, 2) == 1

        def cp(cc, dr, aa_):
            ref = piece(cc, s, aa_, b)
            return rcopy(ref, ref, r1s.at[s, dr, aa_], r1r.at[s, aa_], at_ring(rem(a + (1 if dr == 0 else SIDE - 1), SIDE), b))

        @pl.when(e > 0)
        def _():
            by_core(lambda cc: cp(cc, 0, aa).wait_recv())
        right = jnp.logical_or(e == 0, jnp.logical_and(odd, d < 4))
        left = jnp.logical_or(e == 0, jnp.logical_and(jnp.logical_not(odd), d < 3))

        @pl.when(right)
        def _():
            by_core(lambda cc: cp(cc, 0, aa).start())

        @pl.when(left)
        def _():
            by_core(lambda cc: cp(cc, 1, aa).start())

    def ring1_drain(s):
        @pl.loop(0, 8)
        def _(e):
            aa, d = ap(e)
            odd = lax.rem(e, 2) == 1

            def cp(cc, dr):
                ref = piece(cc, s, aa, b)
                return rcopy(ref, ref, r1s.at[s, dr, aa], r1r.at[s, aa], at_ring(rem(a + 1, SIDE), b))

            @pl.when(jnp.logical_or(e == 0, jnp.logical_and(odd, d < 4)))
            def _():
                by_core(lambda cc: cp(cc, 0).wait_send())

            @pl.when(jnp.logical_or(e == 0, jnp.logical_and(jnp.logical_not(odd), d < 3)))
            def _():
                by_core(lambda cc: cp(cc, 1).wait_send())

    def cp2(cc, s, dr, bb, aa, dl, e):
        ref = piece(cc, s, aa, bb)
        return rcopy(ref, ref, r2s.at[s, dr, dl, e], r2r.at[s, bb, aa], at_ring(a, rem(b + (1 if dr == 0 else SIDE - 1), SIDE)))

    def ring2(s, dl, e, wait):
        aa, _ = ap(e)
        for dr in (0, 1):
            bb = rem(b + (-dl if dr == 0 else dl), SIDE)
            if wait:
                by_core(lambda cc: cp2(cc, s, dr, bb, aa, dl, e).wait_recv())
            go = jnp.logical_or(dl < 3, (e < 4) if dr == 0 else (e >= 4))

            @pl.when(go)
            def _():
                by_core(lambda cc: cp2(cc, s, dr, bb, aa, dl, e).start())

    def pick(typ, e, bb):
        at_y = lax.rem(e, 2) + 4 * (e // 2) + 2 * lax.rem(typ + bb, 2)
        at_x = 2 * e + lax.rem(typ + bb // 2, 2)
        return jnp.where(c == 0, at_y, at_x)

    def ring2q(typ, dl, e, wait):
        for dr in (0, 1):
            bb = rem(b + (-dl if dr == 0 else dl), SIDE)
            aa = pick(typ, e, bb)
            if wait:
                by_core(lambda cc: cp2(cc, 1, dr, bb, aa, dl, 4 * typ + e).wait_recv())
            go = jnp.logical_or(dl < 3, (e < 2) if dr == 0 else (e >= 2))

            @pl.when(go)
            def _():
                by_core(lambda cc: cp2(cc, 1, dr, bb, aa, dl, 4 * typ + e).start())

    def ring2_last(s, e):
        aa, _ = ap(e)
        bb = rem(b + 4, SIDE)
        by_core(lambda cc: cp2(cc, s, 0, bb, aa, 3, e).wait_recv())

    def ring2q_last(typ, e):
        bb = rem(b + 4, SIDE)
        aa = pick(typ, e, bb)
        by_core(lambda cc: cp2(cc, 1, 0, bb, aa, 3, e).wait_recv())

    def ring2_drain(s):
        @pl.loop(0, 32)
        def _(t):
            dl, e = t // 8, lax.rem(t, 8)
            aa, _ = ap(e)
            for dr in (0, 1):
                ee = e if s == 0 else 2 * lax.rem(e, 4)
                go = jnp.logical_or(dl < 3, (ee < 4) if dr == 0 else (ee >= 4))

                @pl.when(go)
                def _():
                    by_core(lambda cc: cp2(cc, s, dr, b, aa, dl, e).wait_send())

    def sib_ref(cc, s, bb):
        w = min(s, 1)
        if cc == 0:
            cols = pl.ds(0, 2 * wid[w][0])
            return W0.at[bb, :, :, cols] if s == 0 else W1.at[s - 1, bb // 2, lax.rem(bb, 2), :, :, cols]
        cols = pl.ds(coff(w, 1, lax.rem(bb, 2)), wid[w][1])
        if s == 0:
            return W0.at[:, bb // 2, :, cols]
        return W1.at[s - 1, :, lax.rem(s - 1 + bb // 2, 2), bb // 4, :, cols]

    def sib(cc, s, bb):
        ref = sib_ref(cc, s, bb)
        return rcopy(ref, ref, sbs.at[s, bb], sbr.at[s, bb], dev(x, y, 1 - c))

    def sib_start(s, bb):
        by_core(lambda cc: sib(cc, s, bb).start())

    def sib_wait(s):
        @pl.loop(0, SIDE)
        def _(bb):
            by_core(lambda cc: sib(1 - cc, s, bb).wait_recv())

    def sib_drain(s):
        @pl.loop(0, SIDE)
        def _(bb):
            by_core(lambda cc: sib(cc, s, bb).wait_send())

    ns = dict(locals())
    return ns


class Parts:
    pass


def kernel(tok, shift, scale, gate, taps, kvin, qin, oin, out, kvs,
           mod, kvsh, qosh,
           W0, W1, st_kv, st_qo, tmp, p0s, p0r, q0s, q0r, r1s, r1r, r2s, r2r, sbs, sbr,
           normed, keys, vals, vpad, local, mixed, hsend, hrecv, relay, pay, ara, red, rsx, part, agy, tot, fin,
           hs, hr, vs, vr, aas, aar, xs, xr, ys, yr, zs, zr, es, er):
    S = Parts()
    S.__dict__.update(gather_parts(kvsh, qosh, W0, W1, st_kv, st_qo, tmp, p0s, p0r, q0s, q0r, r1s, r1r,
                                   r2s, r2r, sbs, sbr))
    r, x, y, c, b = S.r, S.x, S.y, S.c, S.b
    total = 2 * SIDE * SIDE
    n_tok, width, band = 480, 120, 4
    kv_w = W0.reshape(2 * HD, KP)
    q_w = W1.at[0].reshape(HD, KP)
    o_w = W1.at[1].reshape(HD, KP)

    def norm(lo, hi):
        @pl.loop(lo, hi, unroll=2)
        def _(i):
            rows = pl.ds(pl.multiple_of(i * 16, 16), 16)
            v = tok[rows, :].astype(F32)
            center = v - jnp.mean(v, axis=-1, keepdims=True)
            spread = jnp.mean(center * center, axis=-1, keepdims=True)
            res = center * lax.rsqrt(spread + NORM_EPS) * (1.0 + mod[1:2, :]) + mod[0:1, :]
            normed[rows, 0:D] = res.astype(BF16)

    def lanes(i, n):
        return pl.ds(pl.multiple_of(i * n, n), n)

    def value_chunk(i):
        res = mm(normed[...], kv_w[pl.ds(pl.multiple_of(HD + i * 256, 256), 256), :], NT).astype(BF16)
        vals[:, lanes(i, 256)] = res
        wide = res.astype(F32)
        vpad[1:1 + band, :, lanes(i, 256)] = wide.reshape(band, width, 256)
        hsend[0, :, lanes(i, 256)] = wide[0:width].astype(BF16)
        hsend[1, :, lanes(i, 256)] = wide[n_tok - width:].astype(BF16)

    def key_chunk(i):
        res = mm(normed[...], kv_w[lanes(i, 256), :], NT)
        keys[:, lanes(i, 256)] = jnp.maximum(res, 0.0).astype(BF16)

    def q_chunk(i):
        res = mm(normed[...], q_w[lanes(i, 256), :], NT)
        keys[:, lanes(i, 256)] = jnp.maximum(res, 0.0).astype(BF16)

    def block_mask():
        i = lax.broadcasted_iota(jnp.int32, (128, 128), 0) // HEAD
        k = lax.broadcasted_iota(jnp.int32, (128, 128), 1) // HEAD
        return i == k

    def state_group(g):
        k = keys[:, lanes(g, 128)]
        s = mm(k, vals[:, lanes(g, 128)], TN)
        s = jnp.where(block_mask(), s, 0.0)
        s = s[0:32] + s[32:64] + s[64:96] + s[96:128]
        half, gg = g // 5, lax.rem(g, 5)
        pay[half, pl.ds(pl.multiple_of(gg * 32, 32), 32), :] = s
        ks = mm(jnp.ones((8, n_tok), BF16), k, NN)
        pay[half, pl.ds(160 + gg, 1), :] = ks[0:1]

    def halo(k):
        k2 = 2 if k else -2
        return S.rcopy(hsend.at[k], relay.at[k], hs.at[k], hr.at[k], S.dev(x, rem(y + k2, SIDE), c))

    def hop(k):
        k2 = 2 if k else -2
        origin = S.dev(x, rem(y - k2, SIDE), c)["rows"]
        to = rem(origin + (FRAMES if k else total - FRAMES), total)
        has = origin < total - FRAMES if k else origin >= FRAMES
        return S.rcopy(relay.at[k], hrecv.at[k], vs.at[k], vr.at[k], {"rows": to}), has

    def sends(k):
        return r < total - FRAMES if k else r >= FRAMES

    def halo_start():
        for k in (0, 1):
            pl.when(sends(k))(lambda: halo(k).start())

    def halo_relay():
        for k in (0, 1):
            cp, has = hop(k)

            @pl.when(has)
            def _():
                halo(k).wait_recv()
                cp.start()

    def halo_finish():
        for k in (0, 1):
            row = band + 1 if k == 0 else 0

            @pl.when(sends(1 - k))
            def _():
                hop(k)[0].wait_recv()
                vpad[row] = hrecv[k].astype(F32)

            @pl.when(jnp.logical_not(sends(1 - k)))
            def _():
                vpad[row] = jnp.zeros((width, HD), F32)

    def conv_group(g):
        ln = lanes(g, 128)
        tp = taps[:, ln]
        col = lax.broadcasted_iota(jnp.int32, (width, 128), 0)
        acc = [None] * band
        for k in range(band + 2):
            v = vpad[k, :, ln]
            before = jnp.where(col == 0, 0.0, pltpu.roll(v, 1, 0))
            after = jnp.where(col == width - 1, 0.0, pltpu.roll(v, width - 1, 0))
            for o in range(band):
                m = k - o
                if 0 <= m <= 2:
                    term = tp[3 * m:3 * m + 1] * before + tp[3 * m + 1:3 * m + 2] * v + tp[3 * m + 2:3 * m + 3] * after
                    acc[o] = term if acc[o] is None else acc[o] + term
        for o in range(band):
            local[o * width:(o + 1) * width, ln] = acc[o]

    def arm():
        return S.rcopy(pay.at[1 - c], ara, aas, aar, S.dev(x, y, 1 - c))

    def ar_x(m):
        xx = rem(x + m, SIDE)
        return S.rcopy(red.at[xx], rsx.at[x], xs.at[xx], xr.at[x], S.dev(xx, y, c)), xx

    def ar_y(m):
        yy = rem(y + m, SIDE)
        return S.rcopy(part, agy.at[y], ys.at[yy], yr.at[y], S.dev(x, yy, c)), yy

    def ar_z(m):
        xx = rem(x + m, SIDE)
        return S.rcopy(tot, fin.at[c, x], zs.at[xx], zr.at[x], S.dev(xx, y, c)), xx

    def arrived(m, buf, sem, me):
        k = rem(me + m, SIDE)
        pltpu.make_async_copy(buf.at[k], buf.at[k], sem.at[k]).wait()

    def sum8(buf):
        acc = buf[0]
        for k in range(1, SIDE):
            acc = acc + buf[k]
        return acc

    def ar_a():
        arm().start()

    def ar_b():
        arm().wait_recv()
        mine = pay[c] + ara[...]
        for k in range(SIDE):
            red[k] = mine[24 * k:24 * k + 24]
        rsx[x] = red[x]
        for m in range(1, SIDE):
            ar_x(m)[0].start()

    def ar_c():
        for m in range(1, SIDE):
            arrived(m, rsx, xr, x)
        res = sum8(rsx)
        part[...] = res
        agy[y] = res
        for m in range(1, SIDE):
            ar_y(m)[0].start()

    def ar_d():
        for m in range(1, SIDE):
            arrived(m, agy, yr, y)
        res = sum8(agy)
        tot[...] = res
        fin[c, x] = res
        for m in range(1, SIDE):
            ar_z(m)[0].start()

    def fin_copy(h):
        return S.rcopy(fin.at[h], fin.at[h], es, er, S.dev(x, y, 1 - c))

    def ar_e():
        for m in range(1, SIDE):
            k = rem(x + m, SIDE)
            pltpu.make_async_copy(tot, tot, zr.at[k]).wait()
        fin_copy(c).start()

    def ar_drain():
        arm().wait_send()
        for m in range(1, SIDE):
            ar_x(m)[0].wait_send()
            ar_y(m)[0].wait_send()
            ar_z(m)[0].wait_send()
        fin_copy(c).wait_send()
        for k in (0, 1):
            pl.when(sends(k))(lambda: halo(k).wait_send())
            cp, has = hop(k)
            pl.when(has)(lambda: cp.wait_send())

    def state_of(g):
        half, gg = g // 5, g % 5
        rows = []
        for k in range(4):
            at = 32 * gg + 8 * k
            rows.append(fin[half, at // 24, at % 24:at % 24 + 8])
        return jnp.concatenate(rows, axis=0), fin[half, 6, 16 + gg:17 + gg]

    def linear_group(g):
        s, ks = state_of(g)
        for h in range(4):
            kvs[4 * g + h] = s[:, 32 * h:32 * h + 32] / float(n_tok * total)
        mask = block_mask()
        bd = jnp.where(mask, jnp.concatenate([s] * 4, axis=0), 0.0)
        kd = jnp.where(mask, jnp.transpose(jnp.broadcast_to(ks, (128, 128))), 0.0)
        rhs = jnp.concatenate([bd, kd], axis=1)
        hi = rhs.astype(BF16)
        rest = rhs - hi.astype(F32)
        mid = rest.astype(BF16)
        lo = (rest - mid.astype(F32)).astype(BF16)
        q = keys[:, 128 * g:128 * g + 128]
        res = mm(q, hi, NN) + mm(q, mid, NN) + mm(q, lo, NN)
        lin = res[:, 0:128] / (res[:, 128:256] + DENOM_EPS)
        mixed[:, 128 * g:128 * g + 128] = (lin + local[:, 128 * g:128 * g + 128]).astype(BF16)

    def out_chunk(cols, n):
        w = o_w[:, pl.ds(cols, 256)]
        res = mm(mixed[...], w, NN)
        if n < 256:
            res = res[:, :n]
        ln = pl.ds(cols, n)
        out[:, ln] = (tok[:, ln].astype(F32) + mod[2:3, ln] * res).astype(BF16)

    def level(k, m):
        return jnp.where(k == 0, 0, 2 * k - 1 + m), jnp.logical_and(
            jnp.logical_and(k >= 0, k <= 4), jnp.logical_or(m == 0, jnp.logical_and(k >= 1, k <= 3)))

    def drain_first():
        S.phase0_drain(4, S.kv0, p0s, p0r)
        S.phase0_drain(8, S.qo0, q0s, q0r)
        S.ring1_drain(0)
        S.ring1_drain(1)
        S.ring2_drain(0)
        S.sib_drain(0)

    mod[0, :] = shift[...]
    mod[1, :] = scale[...]
    mod[2, :] = gate[...]
    kvsh[:, KP - 128:] = jnp.zeros((20, 128), BF16)
    qosh[:, :, KP - 128:] = jnp.zeros((2, 10, 128), BF16)
    kvsh[:, 0:D] = kvin[...]
    qosh[0, :, 0:D] = qin[...]
    qosh[1, :, 0:D] = oin[...]
    S.barrier()
    S.phase0_start(4, S.kv0, p0s, p0r)
    S.phase0_start(8, S.qo0, q0s, q0r)
    pay[0, 160:192, :] = jnp.zeros((32, 128), F32)
    pay[1, 160:192, :] = jnp.zeros((32, 128), F32)
    normed[:, KP - 128:] = jnp.zeros((n_tok, 128), BF16)
    norm(0, 20)
    S.phase0_wait(4, 0, st_kv, p0r)
    S.build(0, 4, st_kv)

    @pl.loop(0, 64)
    def _(u):
        diag, dl, m = u // 8, 3 - lax.rem(u // 2, 4), lax.rem(u, 2)
        e, valid = level(diag - dl, m)

        @pl.when(jnp.logical_and(valid, dl == 0))
        def _():
            S.ring1(0, e)
            S.ring2(0, 0, e, False)

        @pl.when(jnp.logical_and(valid, dl > 0))
        def _():
            S.ring2(0, dl, e, True)

        @pl.when(jnp.logical_and(valid, e == 7))
        def _():
            S.sib_start(0, rem(b - dl, SIDE))

            @pl.when(dl > 0)
            def _():
                S.sib_start(0, rem(b + dl, SIDE))

        @pl.when(u == 1)
        def _():
            norm(20, 24)

        @pl.when(u == 9)
        def _():
            norm(24, 30)

        @pl.when(u == 17)
        def _():
            S.phase0_wait(8, 1, st_qo, q0r)
            S.build(1, 8, st_qo)

        step = diag - 3
        for m2 in (0, 1):
            e2, ok = level(step, jnp.int32(m2))

            @pl.when(jnp.logical_and(ok, lax.rem(u, 8) == 0))
            def _():
                S.ring1(1, e2)

    @pl.loop(0, 4)
    def _(e):
        S.ring2q(0, 0, e, False)
        S.ring2_last(0, e)
        S.ring2_last(0, e + 4)
    S.sib_start(0, rem(b + 4, SIDE))
    S.sib_start(1, b)
    S.sib_start(2, b)
    S.sib_wait(0)

    @pl.loop(0, 24)
    def _(u):
        typ, dl, e = u // 12, 1 + lax.rem(u // 4, 3), lax.rem(u, 4)

        @pl.when(u == 12)
        def _():
            @pl.loop(0, 4)
            def _(k):
                S.ring2q(1, 0, k, False)
        S.ring2q(typ, dl, e, True)

        for ty in (0, 1):
            @pl.when(jnp.logical_and(e == 3, typ == ty))
            def _():
                S.sib_start(1 + ty, rem(b - dl, SIDE))
                S.sib_start(1 + ty, rem(b + dl, SIDE))

        @pl.when(jnp.logical_and(u >= 12, u < 16))
        def _():
            S.ring2q_last(0, e)

        @pl.when(u == 15)
        def _():
            S.sib_start(1, rem(b + 4, SIDE))

        @pl.when(u < 5)
        def _():
            value_chunk(u)

        pl.when(u == 4)(halo_start)

        @pl.when(jnp.logical_and(u >= 5, u < 10))
        def _():
            key_chunk(u - 5)

        @pl.when(jnp.logical_and(u >= 10, u < 12))
        def _():
            @pl.loop(0, 5)
            def _(k):
                state_group(5 * (u - 10) + k)

        pl.when(u == 10)(halo_relay)
        pl.when(u == 11)(ar_a)
        pl.when(u == 12)(ar_b)
        pl.when(u == 15)(ar_c)
        pl.when(u == 18)(ar_d)
        pl.when(u == 17)(drain_first)

        @pl.when(u == 19)
        def _():
            S.sib_wait(1)

        @pl.when(u >= 19)
        def _():
            q_chunk(u - 19)

        pl.when(u == 21)(ar_e)

    halo_finish()

    @pl.loop(0, 10)
    def _(g):
        conv_group(g)

    @pl.loop(0, 4)
    def _(e):
        S.ring2q_last(1, e)
    S.sib_start(2, rem(b + 4, SIDE))
    fin_copy(1 - c).wait_recv()
    for g in range(HD // 128):
        linear_group(g)
    S.sib_wait(2)

    @pl.loop(0, 8)
    def _(i):
        out_chunk(pl.multiple_of(i * 256, 256), 256)
    out_chunk(2048, 192)
    ar_drain()
    S.ring2_drain(1)
    S.sib_drain(1)
    S.sib_drain(2)


def body(tokens, shift, scale, gate, query_weight, pair_weight, output_weight, depth_taps):
    band, width, model = tokens.shape
    n = band * width
    dma = pltpu.SemaphoreType.DMA
    vm = pltpu.VMEM
    out, kvs = pl.pallas_call(
        kernel,
        out_shape=(jax.ShapeDtypeStruct((n, model), BF16), jax.ShapeDtypeStruct((HEADS, HEAD, HEAD), F32)),
        in_specs=[pl.BlockSpec(memory_space=vm)] * 8,
        out_specs=[pl.BlockSpec(memory_space=vm)] * 2,
        scratch_shapes=[
            vm((3, model), F32), vm((20, KP), BF16), vm((2, 10, KP), BF16),
            vm((SIDE, 4, UNIT, KP), BF16), vm((2, SIDE // 2, 2, 2, UNIT, KP), BF16),
            vm((4, 20, WIDTHS[0][0]), BF16), vm((8, 10, WMAX), BF16), vm((UNIT, WMAX), F32),
            dma((4,)), dma((4,)), dma((8,)), dma((8,)),
            dma((2, 2, 8)), dma((2, 8)), dma((2, 2, 4, 8)), dma((2, 8, 8)), dma((3, 8)), dma((3, 8)),
            vm((n, KP), BF16), vm((n, HD), BF16), vm((n, HD), BF16), vm((band + 2, width, HD), F32),
            vm((n, HD), F32), vm((n, HD), BF16), vm((2, width, HD), BF16), vm((2, width, HD), BF16), vm((2, width, HD), BF16),
            vm((2, 192, 128), F32), vm((192, 128), F32), vm((SIDE, 24, 128), F32), vm((SIDE, 24, 128), F32),
            vm((24, 128), F32), vm((SIDE, 24, 128), F32), vm((24, 128), F32), vm((2, SIDE, 24, 128), F32),
            dma((2,)), dma((2,)), dma((2,)), dma((2,)), dma, dma, dma((8,)), dma((8,)), dma((8,)), dma((8,)), dma((8,)), dma((8,)), dma, dma,
        ],
        compiler_params=pltpu.CompilerParams(collective_id=0, has_side_effects=True, vmem_limit_bytes=62 << 20),
    )(
        tokens.reshape(n, model), shift, scale, gate, depth_taps,
        pair_weight.T, query_weight.T, output_weight,
    )
    return out.reshape(band, width, model), kvs


def solution(mesh):
    in_specs = (
        P(("clips", "rows"), None, None),
        P("clips"),
        P("clips"),
        P("clips"),
        P(None, "rows"),
        P(None, "rows"),
        P("rows", None),
        P(),
    )
    out_specs = (P(("clips", "rows"), None, None), P("clips", None, None))
    return jax.shard_map(body, mesh=mesh, in_specs=in_specs, out_specs=out_specs, check_vma=False)
```

```python
import jax
import jax.numpy as jnp
from jax import lax
from jax.experimental import pallas as pl
from jax.experimental.pallas import tpu as pltpu
from jax.sharding import PartitionSpec as P

HEADS, HEAD, FRAMES, HD = 40, 32, 8, 1280
NORM_EPS = 1e-06
DENOM_EPS = 1e-06
SIDE = 8
UNIT = 80
D = 2240
KP = 2304
WIDTHS = ((640, 512), (896, 256))
WMAX = 896
F32, BF16 = jnp.float32, jnp.bfloat16
NT = (((1,), (1,)), ((), ()))
TN = (((0,), (0,)), ((), ()))
NN = (((1,), (0,)), ((), ()))


def mm(lhs, rhs, dims):
    return lax.dot_general(lhs, rhs, dims, preferred_element_type=F32)


def rem(v, m):
    return lax.rem(v + m, m)


def gather_parts(kvsh, qosh, W0, W1, st_kv, st_qo, tmp, p0s, p0r, q0s, q0r, r1s, r1r, r2s, r2r, sbs, sbr, pzs):
    r = lax.axis_index("rows")
    c = lax.rem(r, 2)
    y = lax.rem(r // 2, SIDE)
    x = r // (2 * SIDE)
    j, p = y // 2, lax.rem(y, 2)
    i4 = y // 4
    a = jnp.where(c == 0, y, x)
    b = jnp.where(c == 0, x, y)
    wid = WIDTHS
    clip = lax.axis_index("clips")
    zp = lax.rem(clip, 2)
    pair = {"clips": clip + 1 - 2 * zp, "rows": r}

    def dev(xx, yy, cc):
        return {"rows": (xx * SIDE + yy) * 2 + cc}

    def at_ring(aa, bb):
        xx = jnp.where(c == 0, bb, aa)
        yy = jnp.where(c == 0, aa, bb)
        return dev(xx, yy, c)

    def by_core(fn):
        for cc in (0, 1):
            @pl.when(c == cc)
            def _(cc=cc):
                fn(cc)

    def coff(s, cc, pp):
        return pl.multiple_of(cc * 2 * wid[s][0] + pp * wid[s][cc], 128)

    def piece(cc, s, aa, bb):
        xx, yy = (bb, aa) if cc == 0 else (aa, bb)
        cols = pl.ds(coff(s, cc, lax.rem(yy, 2)), wid[s][cc])
        if s == 0:
            return W0.at[xx, yy // 2, :, cols]
        return W1.at[lax.rem(yy // 2 + xx, 2), xx // 2, lax.rem(xx, 2), yy // 4, :, cols]

    def barrier():
        sem = pltpu.get_barrier_semaphore()
        n = 0
        for m in range(1, 8):
            q = lax.rem(lax.rem(y, 4) * 2 + c + m, 8)
            pl.semaphore_signal(sem, inc=1, device_id=dev(x, 4 * i4 + q // 2, lax.rem(q, 2)))
            pl.semaphore_signal(sem, inc=1, device_id=dev(rem(x + m, SIDE), y, c))
            pl.semaphore_signal(sem, inc=1, device_id=dev(x, rem(y + m, SIDE), c))
            n += 3
        for k in (1, -1):
            pl.semaphore_signal(sem, inc=1, device_id=dev(rem(x + k, SIDE), rem(y + 2 * k, SIDE), c))
            n += 1
        pl.semaphore_signal(sem, inc=1, device_id=pair)
        pl.semaphore_wait(sem, n + 1)

    def rcopy(src, dst, ss, rs, d):
        return pltpu.make_async_remote_copy(src_ref=src, dst_ref=dst, send_sem=ss, recv_sem=rs, device_id=d,
                                            device_id_type=pl.DeviceIdType.MESH)

    def kv0(m):
        pd, cd = m // 2, m % 2
        w = wid[0][cd]
        src = kvsh.at[:, pl.ds(cd * 2 * wid[0][0] + pd * w, w)]
        slot = 2 * p + c
        dst = st_kv.at[slot, :, pl.ds(0, w)]
        return src, dst, slot, dev(x, 2 * j + pd, cd), (2 * p + c) == m

    def qo0(m):
        yd, cd = m // 2, m % 2
        pd, td = yd % 2, lax.rem(yd // 2 + x, 2)
        w = wid[1][cd]
        src = qosh.at[td, :, pl.ds(cd * 2 * wid[1][0] + pd * w, w)]
        slot = lax.rem(y, 4) * 2 + c
        dst = st_qo.at[slot, :, pl.ds(0, w)]
        return src, dst, slot, dev(x, 4 * i4 + yd, cd), slot == m

    def phase0_start(n, what, ss, rs):
        for m in range(n):
            src, dst, slot, d, own = what(m)

            @pl.when(own)
            def _():
                pltpu.make_async_copy(src, dst, rs.at[m]).start()

            @pl.when(jnp.logical_not(own))
            def _():
                rcopy(src, dst, ss.at[m], rs.at[slot], d).start()

    def phase0_wait(n, s, stage, rs):
        for m in range(n):
            def w(cc):
                ref = stage.at[m, :, pl.ds(0, wid[s][cc])]
                pltpu.make_async_copy(ref, ref, rs.at[m]).wait()
            by_core(w)

    def phase0_drain(n, what, ss, rs):
        for m in range(n):
            src, dst, slot, d, own = what(m)

            @pl.when(jnp.logical_not(own))
            def _():
                rcopy(src, dst, ss.at[m], rs.at[slot], d).wait_send()

    def build(s, n, stage):
        rows = UNIT // n
        for m in range(n):
            tmp[m * rows:(m + 1) * rows, 0:stage.shape[-1]] = stage[m].astype(jnp.float32)

        def put(cc):
            piece(cc, s, a, b)[...] = tmp[:, :wid[s][cc]].astype(jnp.bfloat16)
        by_core(put)

    def ap(e):
        d = (e + 1) // 2
        return rem(a + jnp.where(lax.rem(e, 2) == 1, -d, d), SIDE), d

    def r1copy(cc, s, k, aa, to):
        ref = piece(cc, s, aa, b)
        return rcopy(ref, ref, r1s.at[s, k], r1r.at[s, aa], at_ring(rem(a + to, SIDE), b))

    def ring1(s, e):
        aa, d = ap(e)

        @pl.when(e > 0)
        def _():
            by_core(lambda cc: r1copy(cc, s, 0, aa, 1).wait_recv())

        if s == 0:
            plan = ((0, 0, 1), (0, 1, -1), (0, 2, 2), (0, 3, -2), (3, 4, 1), (3, 5, 2), (4, 6, -1))
        else:
            plan = ((0, 0, 1), (0, 1, -1), (1, 2, 1), (2, 3, -1), (3, 4, 1), (4, 5, -1), (5, 6, 1))
        for when, k, to in plan:
            @pl.when(e == when)
            def _():
                by_core(lambda cc: r1copy(cc, s, k, aa, to).start())

    def ring1_drain(s):
        @pl.loop(0, 7)
        def _(k):
            by_core(lambda cc: r1copy(cc, s, k, a, 1).wait_send())

    def cp2(cc, s, dr, bb, aa, dl, e):
        ref = piece(cc, s, aa, bb)
        return rcopy(ref, ref, r2s.at[s, dr, dl, e], r2r.at[s, bb, aa], at_ring(a, rem(b + (1 if dr == 0 else SIDE - 1), SIDE)))

    def by_pair(s, typ, e, plane):
        if s == 0:
            return lax.rem(e, 4) == 1 + plane
        return e == 1 + lax.rem(typ + plane, 2)

    def onward(s, typ, dl, e, dr):
        low = e < (4 if s == 0 else 2)
        near = low if dr == 0 else jnp.logical_not(low)
        return jnp.logical_and(jnp.logical_not(by_pair(s, typ, e, zp)), jnp.logical_or(dl < 3, near))

    def zcopy(cc, s, aa, bb, k, e):
        ref = piece(cc, s, aa, bb)
        return rcopy(ref, ref, pzs.at[s, k, e], r2r.at[s, bb, aa], pair)

    def pick(s, typ, e, bb):
        if s == 0:
            return ap(e)[0]
        at_y = lax.rem(e, 2) + 4 * (e // 2) + 2 * lax.rem(typ + bb, 2)
        at_x = 2 * e + lax.rem(typ + bb // 2, 2)
        return jnp.where(c == 0, at_y, at_x)

    def step2(s, typ, dl, e, wait):
        e8 = 4 * typ + e
        for dr in (0, 1):
            bb = rem(b + (-dl if dr == 0 else dl), SIDE)
            aa = pick(s, typ, e, bb)
            if wait:
                @pl.when(jnp.logical_not(by_pair(s, typ, e, zp)))
                def _():
                    by_core(lambda cc: cp2(cc, s, dr, bb, aa, dl, e8).wait_recv())

            @pl.when(onward(s, typ, dl, e, dr))
            def _():
                by_core(lambda cc: cp2(cc, s, dr, bb, aa, dl, e8).start())
            if wait:
                @pl.when(by_pair(s, typ, e, 1 - zp))
                def _():
                    by_core(lambda cc: zcopy(cc, s, aa, bb, 2 * dl - 2 + dr, e8).start())

    def last2(s, typ, e):
        e8 = 4 * typ + e
        bb = rem(b + 4, SIDE)
        aa = pick(s, typ, e, bb)

        @pl.when(jnp.logical_not(by_pair(s, typ, e, zp)))
        def _():
            by_core(lambda cc: cp2(cc, s, 0, bb, aa, 3, e8).wait_recv())

        @pl.when(by_pair(s, typ, e, 1 - zp))
        def _():
            by_core(lambda cc: zcopy(cc, s, aa, bb, 6, e8).start())

    def paired(typ, d):
        bb = rem(b + d, SIDE)
        e = 1 + lax.rem(typ + zp, 2)
        aa = pick(1, typ, e, bb)
        by_core(lambda cc: cp2(cc, 1, 0, bb, aa, 3, 4 * typ + e).wait_recv())

    def paired0(d):
        bb = rem(b + d, SIDE)
        for k in (0, 4):
            e = k + 1 + zp
            aa = pick(0, 0, e, bb)
            by_core(lambda cc: cp2(cc, 0, 0, bb, aa, 3, e).wait_recv())

    def ring2(s, dl, e, wait):
        step2(0, 0, dl, e, wait)

    def ring2_last(s, e):
        last2(0, 0, e)

    def ring2q(typ, dl, e, wait):
        step2(1, typ, dl, e, wait)

    def ring2q_last(typ, e):
        last2(1, typ, e)

    def ring2_drain(s):
        @pl.loop(0, 32)
        def _(t):
            dl, e8 = t // 8, lax.rem(t, 8)
            e, typ = (e8, 0) if s == 0 else (lax.rem(e8, 4), e8 // 4)
            for dr in (0, 1):
                @pl.when(onward(s, typ, dl, e, dr))
                def _():
                    by_core(lambda cc: cp2(cc, s, dr, b, a, dl, e8).wait_send())

        @pl.loop(0, 56)
        def _(t):
            k, e8 = t // 8, lax.rem(t, 8)
            e, typ = (e8, 0) if s == 0 else (lax.rem(e8, 4), e8 // 4)

            @pl.when(by_pair(s, typ, e, 1 - zp))
            def _():
                by_core(lambda cc: zcopy(cc, s, a, b, k, e8).wait_send())

    def sib_ref(cc, s, bb):
        w = min(s, 1)
        if cc == 0:
            cols = pl.ds(0, 2 * wid[w][0])
            return W0.at[bb, :, :, cols] if s == 0 else W1.at[s - 1, bb // 2, lax.rem(bb, 2), :, :, cols]
        cols = pl.ds(coff(w, 1, lax.rem(bb, 2)), wid[w][1])
        if s == 0:
            return W0.at[:, bb // 2, :, cols]
        return W1.at[s - 1, :, lax.rem(s - 1 + bb // 2, 2), bb // 4, :, cols]

    def sib(cc, s, bb):
        ref = sib_ref(cc, s, bb)
        return rcopy(ref, ref, sbs.at[s, bb], sbr.at[s, bb], dev(x, y, 1 - c))

    def sib_start(s, bb):
        by_core(lambda cc: sib(cc, s, bb).start())

    def sib_wait(s):
        @pl.loop(0, SIDE)
        def _(bb):
            by_core(lambda cc: sib(1 - cc, s, bb).wait_recv())

    def sib_drain(s):
        @pl.loop(0, SIDE)
        def _(bb):
            by_core(lambda cc: sib(cc, s, bb).wait_send())

    ns = dict(locals())
    return ns


class Parts:
    pass


def kernel(tok, shift, scale, gate, taps, kvin, qin, oin, out, kvs,
           mod, kvsh, qosh,
           W0, W1, st_kv, st_qo, tmp, p0s, p0r, q0s, q0r, r1s, r1r, r2s, r2r, sbs, sbr, pzs,
           normed, keys, vals, vpad, local, mixed, hsend, hrecv, relay, pay, ara, red, rsx, part, agy, tot, fin,
           hs, hr, vs, vr, aas, aar, xs, xr, ys, yr, zs, zr, es, er):
    S = Parts()
    S.__dict__.update(gather_parts(kvsh, qosh, W0, W1, st_kv, st_qo, tmp, p0s, p0r, q0s, q0r, r1s, r1r,
                                   r2s, r2r, sbs, sbr, pzs))
    r, x, y, c, a, b = S.r, S.x, S.y, S.c, S.a, S.b
    total = 2 * SIDE * SIDE
    n_tok, width, band = 480, 120, 4
    kv_w = W0.reshape(2 * HD, KP)
    q_w = W1.at[0].reshape(HD, KP)
    o_w = W1.at[1].reshape(HD, KP)

    def norm(lo, hi):
        @pl.loop(lo, hi, unroll=2)
        def _(i):
            rows = pl.ds(pl.multiple_of(i * 16, 16), 16)
            v = tok[rows, :].astype(F32)
            center = v - jnp.mean(v, axis=-1, keepdims=True)
            spread = jnp.mean(center * center, axis=-1, keepdims=True)
            res = center * lax.rsqrt(spread + NORM_EPS) * (1.0 + mod[1:2, :]) + mod[0:1, :]
            normed[rows, 0:D] = res.astype(BF16)

    def lanes(i, n):
        return pl.ds(pl.multiple_of(i * n, n), n)

    def value_chunk(i):
        res = mm(normed[...], kv_w[pl.ds(pl.multiple_of(HD + i * 256, 256), 256), :], NT).astype(BF16)
        vals[:, lanes(i, 256)] = res
        wide = res.astype(F32)
        vpad[1:1 + band, :, lanes(i, 256)] = wide.reshape(band, width, 256)
        hsend[0, :, lanes(i, 256)] = wide[0:width].astype(BF16)
        hsend[1, :, lanes(i, 256)] = wide[n_tok - width:].astype(BF16)

    def key_chunk(i):
        res = mm(normed[...], kv_w[lanes(i, 256), :], NT)
        keys[:, lanes(i, 256)] = jnp.maximum(res, 0.0).astype(BF16)

    def q_chunk(i):
        res = mm(normed[...], q_w[lanes(i, 256), :], NT)
        keys[:, lanes(i, 256)] = jnp.maximum(res, 0.0).astype(BF16)

    def block_mask():
        i = lax.broadcasted_iota(jnp.int32, (128, 128), 0) // HEAD
        k = lax.broadcasted_iota(jnp.int32, (128, 128), 1) // HEAD
        return i == k

    def state_group(g):
        k = keys[:, lanes(g, 128)]
        s = mm(k, vals[:, lanes(g, 128)], TN)
        s = jnp.where(block_mask(), s, 0.0)
        s = s[0:32] + s[32:64] + s[64:96] + s[96:128]
        half, gg = g // 5, lax.rem(g, 5)
        pay[half, pl.ds(pl.multiple_of(gg * 32, 32), 32), :] = s
        ks = mm(jnp.ones((8, n_tok), BF16), k, NN)
        pay[half, pl.ds(160 + gg, 1), :] = ks[0:1]

    def halo(k, i):
        k2 = 2 if k else -2
        ln = lanes(i, 256)
        return S.rcopy(hsend.at[k, :, ln], relay.at[k, :, ln], hs.at[k, i], hr.at[k, i],
                       S.dev(x, rem(y + k2, SIDE), c))

    def hop(k, i):
        k2 = 2 if k else -2
        ln = lanes(i, 256)
        origin = S.dev(x, rem(y - k2, SIDE), c)["rows"]
        to = rem(origin + (FRAMES if k else total - FRAMES), total)
        has = origin < total - FRAMES if k else origin >= FRAMES
        return S.rcopy(relay.at[k, :, ln], hrecv.at[k, :, ln], vs.at[k, i], vr.at[k, i], {"rows": to}), has

    def sends(k):
        return r < total - FRAMES if k else r >= FRAMES

    def halo_start(i):
        for k in (0, 1):
            pl.when(sends(k))(lambda: halo(k, i).start())

    def halo_relay(i):
        for k in (0, 1):
            cp, has = hop(k, i)

            @pl.when(has)
            def _():
                halo(k, i).wait_recv()
                cp.start()

    def halo_finish():
        for k in (0, 1):
            row = band + 1 if k == 0 else 0

            @pl.when(sends(1 - k))
            def _():
                @pl.loop(0, 5)
                def _(i):
                    hop(k, i)[0].wait_recv()
                vpad[row] = hrecv[k].astype(F32)

            @pl.when(jnp.logical_not(sends(1 - k)))
            def _():
                vpad[row] = jnp.zeros((width, HD), F32)

    def halo_drain():
        @pl.loop(0, 5)
        def _(i):
            for k in (0, 1):
                pl.when(sends(k))(lambda: halo(k, i).wait_send())
                cp, has = hop(k, i)
                pl.when(has)(lambda: cp.wait_send())

    def conv_group(g):
        ln = lanes(g, 128)
        tp = taps[:, ln]
        col = lax.broadcasted_iota(jnp.int32, (width, 128), 0)
        acc = [None] * band
        for k in range(band + 2):
            v = vpad[k, :, ln]
            before = jnp.where(col == 0, 0.0, pltpu.roll(v, 1, 0))
            after = jnp.where(col == width - 1, 0.0, pltpu.roll(v, width - 1, 0))
            for o in range(band):
                m = k - o
                if 0 <= m <= 2:
                    term = tp[3 * m:3 * m + 1] * before + tp[3 * m + 1:3 * m + 2] * v + tp[3 * m + 2:3 * m + 3] * after
                    acc[o] = term if acc[o] is None else acc[o] + term
        for o in range(band):
            local[o * width:(o + 1) * width, ln] = acc[o]

    def arm():
        return S.rcopy(pay.at[1 - c], ara, aas, aar, S.dev(x, y, 1 - c))

    def ar_x(m):
        k = rem(a + m, SIDE)
        return S.rcopy(red.at[k], rsx.at[a], xs.at[k], xr.at[a], S.at_ring(k, b))

    def ar_y(m):
        k = rem(b + m, SIDE)
        return S.rcopy(part, agy.at[b], ys.at[k], yr.at[b], S.at_ring(a, k))

    def ar_z(m):
        k = rem(a + m, SIDE)
        return S.rcopy(tot, fin.at[c, a], zs.at[k], zr.at[a], S.at_ring(k, b))

    def arrived(m, buf, sem, me):
        k = rem(me + m, SIDE)
        pltpu.make_async_copy(buf.at[k], buf.at[k], sem.at[k]).wait()

    def sum8(buf):
        acc = buf[0]
        for k in range(1, SIDE):
            acc = acc + buf[k]
        return acc

    def ar_a():
        arm().start()

    def ar_b():
        arm().wait_recv()
        mine = pay[c] + ara[...]
        for k in range(SIDE):
            red[k] = mine[24 * k:24 * k + 24]
        rsx[a] = red[a]
        for m in range(1, SIDE):
            ar_x(m).start()

    def ar_c():
        for m in range(1, SIDE):
            arrived(m, rsx, xr, a)
        res = sum8(rsx)
        part[...] = res
        agy[b] = res
        for m in range(1, SIDE):
            ar_y(m).start()

    def ar_d():
        for m in range(1, SIDE):
            arrived(m, agy, yr, b)
        res = sum8(agy)
        tot[...] = res
        fin[c, a] = res
        for m in range(1, SIDE):
            ar_z(m).start()

    def fin_copy(h):
        return S.rcopy(fin.at[h], fin.at[h], es, er, S.dev(x, y, 1 - c))

    def ar_e():
        for m in range(1, SIDE):
            k = rem(a + m, SIDE)
            pltpu.make_async_copy(tot, tot, zr.at[k]).wait()
        fin_copy(c).start()

    def ar_drain():
        arm().wait_send()
        for m in range(1, SIDE):
            ar_x(m).wait_send()
            ar_y(m).wait_send()
            ar_z(m).wait_send()
        fin_copy(c).wait_send()
        halo_drain()

    def state_of(g):
        half, gg = g // 5, g % 5
        rows = []
        for k in range(4):
            at = 32 * gg + 8 * k
            rows.append(fin[half, at // 24, at % 24:at % 24 + 8])
        return jnp.concatenate(rows, axis=0), fin[half, 6, 16 + gg:17 + gg]

    def linear_group(g):
        s, ks = state_of(g)
        for h in range(4):
            kvs[4 * g + h] = s[:, 32 * h:32 * h + 32] / float(n_tok * total)
        mask = block_mask()
        bd = jnp.where(mask, jnp.concatenate([s] * 4, axis=0), 0.0)
        kd = jnp.where(mask, jnp.transpose(jnp.broadcast_to(ks, (128, 128))), 0.0)
        rhs = jnp.concatenate([bd, kd], axis=1)
        hi = rhs.astype(BF16)
        rest = rhs - hi.astype(F32)
        mid = rest.astype(BF16)
        lo = (rest - mid.astype(F32)).astype(BF16)
        q = keys[:, 128 * g:128 * g + 128]
        res = mm(q, hi, NN) + mm(q, mid, NN) + mm(q, lo, NN)
        lin = res[:, 0:128] / (res[:, 128:256] + DENOM_EPS)
        mixed[:, 128 * g:128 * g + 128] = (lin + local[:, 128 * g:128 * g + 128]).astype(BF16)

    def out_chunk(cols, n):
        w = o_w[:, pl.ds(cols, 256)]
        res = mm(mixed[...], w, NN)
        if n < 256:
            res = res[:, :n]
        ln = pl.ds(cols, n)
        out[:, ln] = (tok[:, ln].astype(F32) + mod[2:3, ln] * res).astype(BF16)

    def level(k, m):
        return jnp.where(k == 0, 0, 2 * k - 1 + m), jnp.logical_and(
            jnp.logical_and(k >= 0, k <= 4), jnp.logical_or(m == 0, jnp.logical_and(k >= 1, k <= 3)))

    def drain_first():
        S.phase0_drain(4, S.kv0, p0s, p0r)
        S.phase0_drain(8, S.qo0, q0s, q0r)
        S.ring1_drain(0)
        S.ring1_drain(1)
        S.ring2_drain(0)
        S.sib_drain(0)

    mod[0, :] = shift[...]
    mod[1, :] = scale[...]
    mod[2, :] = gate[...]
    kvsh[:, KP - 128:] = jnp.zeros((20, 128), BF16)
    qosh[:, :, KP - 128:] = jnp.zeros((2, 10, 128), BF16)
    kvsh[:, 0:D] = kvin[...]
    qosh[0, :, 0:D] = qin[...]
    qosh[1, :, 0:D] = oin[...]
    S.barrier()
    S.phase0_start(4, S.kv0, p0s, p0r)
    S.phase0_start(8, S.qo0, q0s, q0r)
    pay[0, 160:192, :] = jnp.zeros((32, 128), F32)
    pay[1, 160:192, :] = jnp.zeros((32, 128), F32)
    normed[:, KP - 128:] = jnp.zeros((n_tok, 128), BF16)
    norm(0, 20)
    S.phase0_wait(4, 0, st_kv, p0r)
    S.build(0, 4, st_kv)

    @pl.loop(0, 64)
    def _(u):
        diag, dl, m = u // 8, 3 - lax.rem(u // 2, 4), lax.rem(u, 2)
        e, valid = level(diag - dl, m)

        @pl.when(jnp.logical_and(valid, dl == 0))
        def _():
            S.ring1(0, e)
            S.ring2(0, 0, e, False)

        @pl.when(jnp.logical_and(valid, dl > 0))
        def _():
            S.ring2(0, dl, e, True)

        @pl.when(jnp.logical_and(valid, e == 7))
        def _():
            @pl.when(dl == 0)
            def _():
                S.sib_start(0, b)

        @pl.when(jnp.logical_and(lax.rem(u, 8) == 7, diag >= 6))
        def _():
            for d in (SIDE + 5 - diag, diag - 5):
                S.paired0(d)
                S.sib_start(0, rem(b + d, SIDE))

        @pl.when(u == 1)
        def _():
            norm(20, 24)

        @pl.when(u == 9)
        def _():
            norm(24, 30)

        @pl.when(u == 17)
        def _():
            S.phase0_wait(8, 1, st_qo, q0r)
            S.build(1, 8, st_qo)

        step = diag - 3
        for m2 in (0, 1):
            e2, ok = level(step, jnp.int32(m2))

            @pl.when(jnp.logical_and(ok, lax.rem(u, 8) == 0))
            def _():
                S.ring1(1, e2)

    @pl.loop(0, 4)
    def _(e):
        S.ring2q(0, 0, e, False)
        S.ring2_last(0, e)
        S.ring2_last(0, e + 4)
    S.sib_start(1, b)
    S.sib_start(2, b)
    for d in (5, 3, 4):
        S.paired0(d)
        S.sib_start(0, rem(b + d, SIDE))
    S.sib_wait(0)

    @pl.loop(0, 24)
    def _(u):
        typ, dl, e = u // 12, 1 + lax.rem(u // 4, 3), lax.rem(u, 4)

        @pl.when(u == 12)
        def _():
            @pl.loop(0, 4)
            def _(k):
                S.ring2q(1, 0, k, False)
        S.ring2q(typ, dl, e, True)

        @pl.when(jnp.logical_and(u >= 12, u < 16))
        def _():
            S.ring2q_last(0, e)

        for ty in (0, 1):
            group = u // 4 - 2
            d_of = 1 + lax.rem(rem(group, 6), 3)

            @pl.when(jnp.logical_and(jnp.logical_and(e == 1, group >= 0), (group >= 3) == (ty == 1)))
            def _():
                for d in (SIDE - d_of, d_of):
                    S.paired(ty, d)
                    S.sib_start(1 + ty, rem(b + d, SIDE))

        @pl.when(u == 18)
        def _():
            S.paired(0, 4)
            S.sib_start(1, rem(b + 4, SIDE))

        @pl.when(u < 5)
        def _():
            value_chunk(u)

        uh = u - 6 * c

        @pl.when(jnp.logical_and(uh >= 0, uh < 5))
        def _():
            halo_start(uh)

        @pl.when(jnp.logical_and(u >= 5, u < 10))
        def _():
            key_chunk(u - 5)

        @pl.when(jnp.logical_and(jnp.logical_and(uh >= 7, uh < 17), lax.rem(uh, 2) == 1))
        def _():
            halo_relay((uh - 7) // 2)

        @pl.when(jnp.logical_and(u >= 10, u < 12))
        def _():
            @pl.loop(0, 5)
            def _(k):
                state_group(5 * (u - 10) + k)

        pl.when(u == 11)(ar_a)
        pl.when(u == 13)(ar_b)
        pl.when(u == 18)(ar_c)
        pl.when(u == 23)(ar_d)
        pl.when(u == 16)(drain_first)

        @pl.when(u == 19)
        def _():
            S.sib_wait(1)

        @pl.when(u >= 19)
        def _():
            q_chunk(u - 19)

    @pl.loop(0, 4)
    def _(e):
        S.ring2q_last(1, e)
    for d in (6, 2, 5, 3, 4):
        S.paired(1, d)
        S.sib_start(2, rem(b + d, SIDE))
    ar_e()
    halo_finish()

    @pl.loop(0, 10)
    def _(g):
        conv_group(g)
    fin_copy(1 - c).wait_recv()
    for g in range(HD // 128):
        linear_group(g)
    S.sib_wait(2)

    @pl.loop(0, 8)
    def _(i):
        out_chunk(pl.multiple_of(i * 256, 256), 256)
    out_chunk(2048, 192)
    ar_drain()
    S.ring2_drain(1)
    S.sib_drain(1)
    S.sib_drain(2)


def body(tokens, shift, scale, gate, query_weight, pair_weight, output_weight, depth_taps):
    band, width, model = tokens.shape
    n = band * width
    dma = pltpu.SemaphoreType.DMA
    vm = pltpu.VMEM
    out, kvs = pl.pallas_call(
        kernel,
        out_shape=(jax.ShapeDtypeStruct((n, model), BF16), jax.ShapeDtypeStruct((HEADS, HEAD, HEAD), F32)),
        in_specs=[pl.BlockSpec(memory_space=vm)] * 8,
        out_specs=[pl.BlockSpec(memory_space=vm)] * 2,
        scratch_shapes=[
            vm((3, model), F32), vm((20, KP), BF16), vm((2, 10, KP), BF16),
            vm((SIDE, 4, UNIT, KP), BF16), vm((2, SIDE // 2, 2, 2, UNIT, KP), BF16),
            vm((4, 20, WIDTHS[0][0]), BF16), vm((8, 10, WMAX), BF16), vm((UNIT, WMAX), F32),
            dma((4,)), dma((4,)), dma((8,)), dma((8,)),
            dma((2, 7)), dma((2, 8)), dma((2, 2, 4, 8)), dma((2, 8, 8)), dma((3, 8)), dma((3, 8)), dma((2, 7, 8)),
            vm((n, KP), BF16), vm((n, HD), BF16), vm((n, HD), BF16), vm((band + 2, width, HD), F32),
            vm((n, HD), F32), vm((n, HD), BF16), vm((2, width, HD), BF16), vm((2, width, HD), BF16), vm((2, width, HD), BF16),
            vm((2, 192, 128), F32), vm((192, 128), F32), vm((SIDE, 24, 128), F32), vm((SIDE, 24, 128), F32),
            vm((24, 128), F32), vm((SIDE, 24, 128), F32), vm((24, 128), F32), vm((2, SIDE, 24, 128), F32),
            dma((2, 5)), dma((2, 5)), dma((2, 5)), dma((2, 5)), dma, dma, dma((8,)), dma((8,)), dma((8,)), dma((8,)), dma((8,)), dma((8,)), dma, dma,
        ],
        compiler_params=pltpu.CompilerParams(collective_id=0, has_side_effects=True, vmem_limit_bytes=50 << 20),
    )(
        tokens.reshape(n, model), shift, scale, gate, depth_taps,
        pair_weight.T, query_weight.T, output_weight,
    )
    return out.reshape(band, width, model), kvs


def solution(mesh):
    in_specs = (
        P(("clips", "rows"), None, None),
        P("clips"),
        P("clips"),
        P("clips"),
        P(None, "rows"),
        P(None, "rows"),
        P("rows", None),
        P(),
    )
    out_specs = (P(("clips", "rows"), None, None), P("clips", None, None))
    return jax.shard_map(body, mesh=mesh, in_specs=in_specs, out_specs=out_specs, check_vma=False)
```

```python
import jax
import jax.numpy as jnp
from jax import lax
from jax.experimental import pallas as pl
from jax.experimental.pallas import tpu as pltpu
from jax.sharding import PartitionSpec as P

HEADS, HEAD, FRAMES, HD = 40, 32, 8, 1280
NORM_EPS = 1e-06
DENOM_EPS = 1e-06
SIDE = 8
UNIT = 80
D = 2240
KP = 2304
WIDTHS = ((640, 512), (896, 256))
WMAX = 896
F32, BF16 = jnp.float32, jnp.bfloat16
NT = (((1,), (1,)), ((), ()))
TN = (((0,), (0,)), ((), ()))
NN = (((1,), (0,)), ((), ()))


def mm(lhs, rhs, dims):
    return lax.dot_general(lhs, rhs, dims, preferred_element_type=F32)


def rem(v, m):
    return lax.rem(v + m, m)


def gather_parts(kvsh, qosh, W0, W1, st_kv, st_qo, tmp, p0s, p0r, q0s, q0r, r1s, r1r, r2s, r2r, sbs, sbr, pzs):
    r = lax.axis_index("rows")
    c = lax.rem(r, 2)
    y = lax.rem(r // 2, SIDE)
    x = r // (2 * SIDE)
    j, p = y // 2, lax.rem(y, 2)
    i4 = y // 4
    a = jnp.where(c == 0, y, x)
    b = jnp.where(c == 0, x, y)
    wid = WIDTHS
    clip = lax.axis_index("clips")
    zp = lax.rem(clip, 2)
    pair = {"clips": clip + 1 - 2 * zp, "rows": r}

    def dev(xx, yy, cc):
        return {"rows": (xx * SIDE + yy) * 2 + cc}

    def at_ring(aa, bb):
        xx = jnp.where(c == 0, bb, aa)
        yy = jnp.where(c == 0, aa, bb)
        return dev(xx, yy, c)

    def by_core(fn):
        for cc in (0, 1):
            @pl.when(c == cc)
            def _(cc=cc):
                fn(cc)

    def coff(s, cc, pp):
        return pl.multiple_of(cc * 2 * wid[s][0] + pp * wid[s][cc], 128)

    def piece(cc, s, aa, bb):
        xx, yy = (bb, aa) if cc == 0 else (aa, bb)
        cols = pl.ds(coff(s, cc, lax.rem(yy, 2)), wid[s][cc])
        if s == 0:
            return W0.at[xx, yy // 2, :, cols]
        return W1.at[lax.rem(yy // 2 + xx, 2), xx // 2, lax.rem(xx, 2), yy // 4, :, cols]

    def barrier():
        sem = pltpu.get_barrier_semaphore()
        n = 0
        for m in range(1, 8):
            q = lax.rem(lax.rem(y, 4) * 2 + c + m, 8)
            pl.semaphore_signal(sem, inc=1, device_id=dev(x, 4 * i4 + q // 2, lax.rem(q, 2)))
            pl.semaphore_signal(sem, inc=1, device_id=dev(rem(x + m, SIDE), y, c))
            pl.semaphore_signal(sem, inc=1, device_id=dev(x, rem(y + m, SIDE), c))
            n += 3
        for k in (1, -1):
            pl.semaphore_signal(sem, inc=1, device_id=dev(rem(x + k, SIDE), rem(y + 2 * k, SIDE), c))
            n += 1
        pl.semaphore_signal(sem, inc=1, device_id=pair)
        pl.semaphore_wait(sem, n + 1)

    def rcopy(src, dst, ss, rs, d):
        return pltpu.make_async_remote_copy(src_ref=src, dst_ref=dst, send_sem=ss, recv_sem=rs, device_id=d,
                                            device_id_type=pl.DeviceIdType.MESH)

    def kv0(m):
        pd, cd = m // 2, m % 2
        w = wid[0][cd]
        src = kvsh.at[:, pl.ds(cd * 2 * wid[0][0] + pd * w, w)]
        slot = 2 * p + c
        dst = st_kv.at[slot, :, pl.ds(0, w)]
        return src, dst, slot, dev(x, 2 * j + pd, cd), (2 * p + c) == m

    def qo0(m):
        yd, cd = m // 2, m % 2
        pd, td = yd % 2, lax.rem(yd // 2 + x, 2)
        w = wid[1][cd]
        src = qosh.at[td, :, pl.ds(cd * 2 * wid[1][0] + pd * w, w)]
        slot = lax.rem(y, 4) * 2 + c
        dst = st_qo.at[slot, :, pl.ds(0, w)]
        return src, dst, slot, dev(x, 4 * i4 + yd, cd), slot == m

    def phase0_start(n, what, ss, rs):
        for m in range(n):
            src, dst, slot, d, own = what(m)

            @pl.when(own)
            def _():
                pltpu.make_async_copy(src, dst, rs.at[m]).start()

            @pl.when(jnp.logical_not(own))
            def _():
                rcopy(src, dst, ss.at[m], rs.at[slot], d).start()

    def phase0_wait(n, s, stage, rs):
        for m in range(n):
            def w(cc):
                ref = stage.at[m, :, pl.ds(0, wid[s][cc])]
                pltpu.make_async_copy(ref, ref, rs.at[m]).wait()
            by_core(w)

    def phase0_drain(n, what, ss, rs):
        for m in range(n):
            src, dst, slot, d, own = what(m)

            @pl.when(jnp.logical_not(own))
            def _():
                rcopy(src, dst, ss.at[m], rs.at[slot], d).wait_send()

    def build(s, n, stage):
        rows = UNIT // n
        for m in range(n):
            tmp[m * rows:(m + 1) * rows, 0:stage.shape[-1]] = stage[m].astype(jnp.float32)

        def put(cc):
            piece(cc, s, a, b)[...] = tmp[:, :wid[s][cc]].astype(jnp.bfloat16)
        by_core(put)

    def ap(e):
        d = (e + 1) // 2
        return rem(a + jnp.where(lax.rem(e, 2) == 1, -d, d), SIDE), d

    def r1copy(cc, s, k, aa, to):
        ref = piece(cc, s, aa, b)
        return rcopy(ref, ref, r1s.at[s, k], r1r.at[s, aa], at_ring(rem(a + to, SIDE), b))

    def ring1(s, e):
        aa, d = ap(e)

        @pl.when(e > 0)
        def _():
            by_core(lambda cc: r1copy(cc, s, 0, aa, 1).wait_recv())

        if s == 0:
            plan = ((0, 0, 1), (0, 1, -1), (0, 2, 2), (0, 3, -2), (3, 4, 1), (3, 5, 2), (4, 6, -1))
        else:
            plan = ((0, 0, 1), (0, 1, -1), (1, 2, 1), (2, 3, -1), (3, 4, 1), (4, 5, -1), (5, 6, 1))
        for when, k, to in plan:
            @pl.when(e == when)
            def _():
                by_core(lambda cc: r1copy(cc, s, k, aa, to).start())

    def ring1_drain(s):
        @pl.loop(0, 7)
        def _(k):
            by_core(lambda cc: r1copy(cc, s, k, a, 1).wait_send())

    def cp2(cc, s, dr, bb, aa, dl, e):
        ref = piece(cc, s, aa, bb)
        return rcopy(ref, ref, r2s.at[s, dr, dl, e], r2r.at[s, bb, aa], at_ring(a, rem(b + (1 if dr == 0 else SIDE - 1), SIDE)))

    def by_pair(s, typ, e, plane):
        if s == 0:
            return lax.rem(e, 4) == plane
        return e == lax.rem(typ + plane, 2)

    def onward(s, typ, dl, e, dr):
        low = e < (4 if s == 0 else 2)
        near = low if dr == 0 else jnp.logical_not(low)
        return jnp.logical_and(jnp.logical_not(by_pair(s, typ, e, zp)), jnp.logical_or(dl < 3, near))

    def zcopy(cc, s, aa, bb, k, e):
        ref = piece(cc, s, aa, bb)
        return rcopy(ref, ref, pzs.at[s, k, e], r2r.at[s, bb, aa], pair)

    def pick(s, typ, e, bb):
        if s == 0:
            return ap(e)[0]
        at_y = lax.rem(e, 2) + 4 * (e // 2) + 2 * lax.rem(typ + bb, 2)
        at_x = 2 * e + lax.rem(typ + bb // 2, 2)
        return jnp.where(c == 0, at_y, at_x)

    def step2(s, typ, dl, e, wait):
        e8 = 4 * typ + e
        for dr in (0, 1):
            bb = rem(b + (-dl if dr == 0 else dl), SIDE)
            aa = pick(s, typ, e, bb)
            if wait:
                @pl.when(jnp.logical_not(by_pair(s, typ, e, zp)))
                def _():
                    by_core(lambda cc: cp2(cc, s, dr, bb, aa, dl, e8).wait_recv())

            @pl.when(onward(s, typ, dl, e, dr))
            def _():
                by_core(lambda cc: cp2(cc, s, dr, bb, aa, dl, e8).start())
            if wait:
                @pl.when(by_pair(s, typ, e, 1 - zp))
                def _():
                    by_core(lambda cc: zcopy(cc, s, aa, bb, 2 * dl - 2 + dr, e8).start())

    def last2(s, typ, e):
        e8 = 4 * typ + e
        bb = rem(b + 4, SIDE)
        aa = pick(s, typ, e, bb)

        @pl.when(jnp.logical_not(by_pair(s, typ, e, zp)))
        def _():
            by_core(lambda cc: cp2(cc, s, 0, bb, aa, 3, e8).wait_recv())

        @pl.when(by_pair(s, typ, e, 1 - zp))
        def _():
            by_core(lambda cc: zcopy(cc, s, aa, bb, 6, e8).start())

    def paired(typ, d):
        bb = rem(b + d, SIDE)
        e = lax.rem(typ + zp, 2)
        aa = pick(1, typ, e, bb)
        by_core(lambda cc: cp2(cc, 1, 0, bb, aa, 3, 4 * typ + e).wait_recv())

    def paired0(d):
        bb = rem(b + d, SIDE)
        for k in (0, 4):
            e = k + zp
            aa = pick(0, 0, e, bb)
            by_core(lambda cc: cp2(cc, 0, 0, bb, aa, 3, e).wait_recv())

    def ring2(s, dl, e, wait):
        step2(0, 0, dl, e, wait)

    def ring2_last(s, e):
        last2(0, 0, e)

    def ring2q(typ, dl, e, wait):
        step2(1, typ, dl, e, wait)

    def ring2q_last(typ, e):
        last2(1, typ, e)

    def ring2_drain(s):
        @pl.loop(0, 32)
        def _(t):
            dl, e8 = t // 8, lax.rem(t, 8)
            e, typ = (e8, 0) if s == 0 else (lax.rem(e8, 4), e8 // 4)
            for dr in (0, 1):
                @pl.when(onward(s, typ, dl, e, dr))
                def _():
                    by_core(lambda cc: cp2(cc, s, dr, b, a, dl, e8).wait_send())

        @pl.loop(0, 14)
        def _(t):
            k, h = t // 2, lax.rem(t, 2)
            e8 = 4 * h + (1 - zp if s == 0 else lax.rem(h + 1 - zp, 2))
            by_core(lambda cc: zcopy(cc, s, a, b, k, e8).wait_send())

    def sib_ref(cc, s, bb):
        w = min(s, 1)
        if cc == 0:
            cols = pl.ds(0, 2 * wid[w][0])
            return W0.at[bb, :, :, cols] if s == 0 else W1.at[s - 1, bb // 2, lax.rem(bb, 2), :, :, cols]
        cols = pl.ds(coff(w, 1, lax.rem(bb, 2)), wid[w][1])
        if s == 0:
            return W0.at[:, bb // 2, :, cols]
        return W1.at[s - 1, :, lax.rem(s - 1 + bb // 2, 2), bb // 4, :, cols]

    def sib(cc, s, bb):
        ref = sib_ref(cc, s, bb)
        return rcopy(ref, ref, sbs.at[s, bb], sbr.at[s, bb], dev(x, y, 1 - c))

    def sib_start(s, bb):
        by_core(lambda cc: sib(cc, s, bb).start())

    def sib_wait(s):
        @pl.loop(0, SIDE)
        def _(bb):
            by_core(lambda cc: sib(1 - cc, s, bb).wait_recv())

    def sib_drain(s):
        @pl.loop(0, SIDE)
        def _(bb):
            by_core(lambda cc: sib(cc, s, bb).wait_send())

    ns = dict(locals())
    return ns


class Parts:
    pass


def kernel(tok, shift, scale, gate, taps, kvin, qin, oin, out, kvs,
           mod, kvsh, qosh,
           W0, W1, st_kv, st_qo, tmp, p0s, p0r, q0s, q0r, r1s, r1r, r2s, r2r, sbs, sbr, pzs,
           normed, keys, vals, vpad, local, mixed, hsend, hrecv, relay, pay, ara, red, rsx, part, agy, tot, fin,
           hs, hr, vs, vr, aas, aar, xs, xr, ys, yr, zs, zr, es, er):
    S = Parts()
    S.__dict__.update(gather_parts(kvsh, qosh, W0, W1, st_kv, st_qo, tmp, p0s, p0r, q0s, q0r, r1s, r1r,
                                   r2s, r2r, sbs, sbr, pzs))
    r, x, y, c, a, b = S.r, S.x, S.y, S.c, S.a, S.b
    total = 2 * SIDE * SIDE
    n_tok, width, band = 480, 120, 4
    kv_w = W0.reshape(2 * HD, KP)
    q_w = W1.at[0].reshape(HD, KP)
    o_w = W1.at[1].reshape(HD, KP)

    def norm(lo, hi):
        @pl.loop(lo, hi, unroll=2)
        def _(i):
            rows = pl.ds(pl.multiple_of(i * 16, 16), 16)
            v = tok[rows, :].astype(F32)
            center = v - jnp.mean(v, axis=-1, keepdims=True)
            spread = jnp.mean(center * center, axis=-1, keepdims=True)
            res = center * lax.rsqrt(spread + NORM_EPS) * (1.0 + mod[1:2, :]) + mod[0:1, :]
            normed[rows, 0:D] = res.astype(BF16)

    def lanes(i, n):
        return pl.ds(pl.multiple_of(i * n, n), n)

    def value_chunk(i):
        res = mm(normed[...], kv_w[pl.ds(pl.multiple_of(HD + i * 256, 256), 256), :], NT).astype(BF16)
        vals[:, lanes(i, 256)] = res
        wide = res.astype(F32)
        vpad[1:1 + band, :, lanes(i, 256)] = wide.reshape(band, width, 256)
        hsend[0, :, lanes(i, 256)] = wide[0:width].astype(BF16)
        hsend[1, :, lanes(i, 256)] = wide[n_tok - width:].astype(BF16)

    def key_chunk(i):
        res = mm(normed[...], kv_w[lanes(i, 256), :], NT)
        keys[:, lanes(i, 256)] = jnp.maximum(res, 0.0).astype(BF16)

    def q_chunk(i):
        res = mm(normed[...], q_w[lanes(i, 256), :], NT)
        keys[:, lanes(i, 256)] = jnp.maximum(res, 0.0).astype(BF16)

    def block_mask():
        i = lax.broadcasted_iota(jnp.int32, (128, 128), 0) // HEAD
        k = lax.broadcasted_iota(jnp.int32, (128, 128), 1) // HEAD
        return i == k

    def state_group(g):
        k = keys[:, lanes(g, 128)]
        s = mm(k, vals[:, lanes(g, 128)], TN)
        s = jnp.where(block_mask(), s, 0.0)
        s = s[0:32] + s[32:64] + s[64:96] + s[96:128]
        half, gg = g // 5, lax.rem(g, 5)
        pay[half, pl.ds(pl.multiple_of(gg * 32, 32), 32), :] = s
        ks = mm(jnp.ones((8, n_tok), BF16), k, NN)
        pay[half, pl.ds(160 + gg, 1), :] = ks[0:1]

    def halo(k, i):
        k2 = 2 if k else -2
        ln = lanes(i, 256)
        return S.rcopy(hsend.at[k, :, ln], relay.at[k, :, ln], hs.at[k, i], hr.at[k, i],
                       S.dev(x, rem(y + k2, SIDE), c))

    def hop(k, i):
        k2 = 2 if k else -2
        ln = lanes(i, 256)
        origin = S.dev(x, rem(y - k2, SIDE), c)["rows"]
        to = rem(origin + (FRAMES if k else total - FRAMES), total)
        has = origin < total - FRAMES if k else origin >= FRAMES
        return S.rcopy(relay.at[k, :, ln], hrecv.at[k, :, ln], vs.at[k, i], vr.at[k, i], {"rows": to}), has

    def sends(k):
        return r < total - FRAMES if k else r >= FRAMES

    def halo_start(i):
        for k in (0, 1):
            pl.when(sends(k))(lambda: halo(k, i).start())

    def halo_relay(i):
        for k in (0, 1):
            cp, has = hop(k, i)

            @pl.when(has)
            def _():
                halo(k, i).wait_recv()
                cp.start()

    def halo_finish():
        for k in (0, 1):
            row = band + 1 if k == 0 else 0

            @pl.when(sends(1 - k))
            def _():
                @pl.loop(0, 5)
                def _(i):
                    hop(k, i)[0].wait_recv()
                vpad[row] = hrecv[k].astype(F32)

            @pl.when(jnp.logical_not(sends(1 - k)))
            def _():
                vpad[row] = jnp.zeros((width, HD), F32)

    def halo_drain():
        @pl.loop(0, 5)
        def _(i):
            for k in (0, 1):
                pl.when(sends(k))(lambda: halo(k, i).wait_send())
                cp, has = hop(k, i)
                pl.when(has)(lambda: cp.wait_send())

    def conv_group(g):
        ln = lanes(g, 128)
        tp = taps[:, ln]
        col = lax.broadcasted_iota(jnp.int32, (width, 128), 0)
        acc = [None] * band
        for k in range(band + 2):
            v = vpad[k, :, ln]
            before = jnp.where(col == 0, 0.0, pltpu.roll(v, 1, 0))
            after = jnp.where(col == width - 1, 0.0, pltpu.roll(v, width - 1, 0))
            for o in range(band):
                m = k - o
                if 0 <= m <= 2:
                    term = tp[3 * m:3 * m + 1] * before + tp[3 * m + 1:3 * m + 2] * v + tp[3 * m + 2:3 * m + 3] * after
                    acc[o] = term if acc[o] is None else acc[o] + term
        for o in range(band):
            local[o * width:(o + 1) * width, ln] = acc[o]

    def arm():
        return S.rcopy(pay.at[1 - c], ara, aas, aar, S.dev(x, y, 1 - c))

    def ar_x(m):
        k = rem(a + m, SIDE)
        return S.rcopy(red.at[k], rsx.at[a], xs.at[k], xr.at[a], S.at_ring(k, b))

    def ar_y(m):
        k = rem(b + m, SIDE)
        return S.rcopy(part, agy.at[b], ys.at[k], yr.at[b], S.at_ring(a, k))

    def ar_z(m):
        k = rem(a + m, SIDE)
        return S.rcopy(tot, fin.at[c, a], zs.at[k], zr.at[a], S.at_ring(k, b))

    def arrived(m, buf, sem, me):
        k = rem(me + m, SIDE)
        pltpu.make_async_copy(buf.at[k], buf.at[k], sem.at[k]).wait()

    def sum8(buf):
        acc = buf[0]
        for k in range(1, SIDE):
            acc = acc + buf[k]
        return acc

    def ar_a():
        arm().start()

    def ar_b():
        arm().wait_recv()
        mine = pay[c] + ara[...]
        for k in range(SIDE):
            red[k] = mine[24 * k:24 * k + 24]
        rsx[a] = red[a]
        for m in range(1, SIDE):
            ar_x(m).start()

    def ar_c():
        for m in range(1, SIDE):
            arrived(m, rsx, xr, a)
        res = sum8(rsx)
        part[...] = res
        agy[b] = res
        for m in range(1, SIDE):
            ar_y(m).start()

    def ar_d():
        for m in range(1, SIDE):
            arrived(m, agy, yr, b)
        res = sum8(agy)
        tot[...] = res
        fin[c, a] = res
        for m in range(1, SIDE):
            ar_z(m).start()

    def fin_copy(h):
        return S.rcopy(fin.at[h], fin.at[h], es, er, S.dev(x, y, 1 - c))

    def ar_e():
        for m in range(1, SIDE):
            k = rem(a + m, SIDE)
            pltpu.make_async_copy(tot, tot, zr.at[k]).wait()
        fin_copy(c).start()

    def ar_drain():
        arm().wait_send()
        for m in range(1, SIDE):
            ar_x(m).wait_send()
            ar_y(m).wait_send()
            ar_z(m).wait_send()
        fin_copy(c).wait_send()
        halo_drain()

    def state_of(g):
        half, gg = g // 5, g % 5
        rows = []
        for k in range(4):
            at = 32 * gg + 8 * k
            rows.append(fin[half, at // 24, at % 24:at % 24 + 8])
        return jnp.concatenate(rows, axis=0), fin[half, 6, 16 + gg:17 + gg]

    def linear_group(g):
        s, ks = state_of(g)
        for h in range(4):
            kvs[4 * g + h] = s[:, 32 * h:32 * h + 32] / float(n_tok * total)
        mask = block_mask()
        bd = jnp.where(mask, jnp.concatenate([s] * 4, axis=0), 0.0)
        kd = jnp.where(mask, jnp.transpose(jnp.broadcast_to(ks, (128, 128))), 0.0)
        rhs = jnp.concatenate([bd, kd], axis=1)
        hi = rhs.astype(BF16)
        rest = rhs - hi.astype(F32)
        mid = rest.astype(BF16)
        lo = (rest - mid.astype(F32)).astype(BF16)
        q = keys[:, 128 * g:128 * g + 128]
        res = mm(q, hi, NN) + mm(q, mid, NN) + mm(q, lo, NN)
        lin = res[:, 0:128] / (res[:, 128:256] + DENOM_EPS)
        mixed[:, 128 * g:128 * g + 128] = (lin + local[:, 128 * g:128 * g + 128]).astype(BF16)

    def out_chunk(cols, n):
        w = o_w[:, pl.ds(cols, 256)]
        res = mm(mixed[...], w, NN)
        if n < 256:
            res = res[:, :n]
        ln = pl.ds(cols, n)
        out[:, ln] = (tok[:, ln].astype(F32) + mod[2:3, ln] * res).astype(BF16)

    def level(k, m):
        return jnp.where(k == 0, 0, 2 * k - 1 + m), jnp.logical_and(
            jnp.logical_and(k >= 0, k <= 4), jnp.logical_or(m == 0, jnp.logical_and(k >= 1, k <= 3)))

    def drain_first():
        S.phase0_drain(4, S.kv0, p0s, p0r)
        S.phase0_drain(8, S.qo0, q0s, q0r)
        S.ring1_drain(0)
        S.ring1_drain(1)
        S.ring2_drain(0)
        S.sib_drain(0)

    mod[0, :] = shift[...]
    mod[1, :] = scale[...]
    mod[2, :] = gate[...]
    kvsh[:, KP - 128:] = jnp.zeros((20, 128), BF16)
    qosh[:, :, KP - 128:] = jnp.zeros((2, 10, 128), BF16)
    kvsh[:, 0:D] = kvin[...]
    qosh[0, :, 0:D] = qin[...]
    qosh[1, :, 0:D] = oin[...]
    S.barrier()
    S.phase0_start(4, S.kv0, p0s, p0r)
    S.phase0_start(8, S.qo0, q0s, q0r)
    pay[0, 160:192, :] = jnp.zeros((32, 128), F32)
    pay[1, 160:192, :] = jnp.zeros((32, 128), F32)
    normed[:, KP - 128:] = jnp.zeros((n_tok, 128), BF16)
    norm(0, 20)
    S.phase0_wait(4, 0, st_kv, p0r)
    S.build(0, 4, st_kv)

    @pl.loop(0, 64)
    def _(u):
        diag, dl, m = u // 8, 3 - lax.rem(u // 2, 4), lax.rem(u, 2)
        e, valid = level(diag - dl, m)

        @pl.when(jnp.logical_and(valid, dl == 0))
        def _():
            S.ring1(0, e)
            S.ring2(0, 0, e, False)

        @pl.when(jnp.logical_and(valid, dl > 0))
        def _():
            S.ring2(0, dl, e, True)

        @pl.when(jnp.logical_and(valid, e == 7))
        def _():
            @pl.when(dl == 0)
            def _():
                S.sib_start(0, b)

        @pl.when(jnp.logical_and(lax.rem(u, 8) == 7, diag >= 6))
        def _():
            for d in (SIDE + 5 - diag, diag - 5):
                S.paired0(d)
                S.sib_start(0, rem(b + d, SIDE))

        @pl.when(u == 7)
        def _():
            norm(20, 30)

        @pl.when(u == 17)
        def _():
            S.phase0_wait(8, 1, st_qo, q0r)
            S.build(1, 8, st_qo)
            S.ring1(1, jnp.int32(0))

        for m2 in (0, 1):
            e2, ok = level(diag - 3, jnp.int32(m2))

            @pl.when(jnp.logical_and(jnp.logical_and(ok, diag > 3), lax.rem(u, 8) == 7))
            def _():
                S.ring1(1, e2)

    @pl.loop(0, 4)
    def _(e):
        S.ring2q(0, 0, e, False)

    @pl.loop(0, 8)
    def _(e):
        S.ring2_last(0, e)
    S.sib_start(1, b)
    S.sib_start(2, b)
    for d in (5, 3, 4):
        S.paired0(d)
        S.sib_start(0, rem(b + d, SIDE))
    S.sib_wait(0)

    @pl.loop(0, 24)
    def _(u):
        typ, dl, e = u // 12, 1 + lax.rem(u // 4, 3), lax.rem(u, 4)

        @pl.when(u == 12)
        def _():
            @pl.loop(0, 4)
            def _(k):
                S.ring2q(1, 0, k, False)
        S.ring2q(typ, dl, e, True)

        @pl.when(jnp.logical_and(u >= 12, u < 16))
        def _():
            S.ring2q_last(0, e)

        for ty in (0, 1):
            group = u // 4 - 2
            d_of = 1 + lax.rem(rem(group, 6), 3)

            @pl.when(jnp.logical_and(jnp.logical_and(e == 1, group >= 0), (group >= 3) == (ty == 1)))
            def _():
                for d in (SIDE - d_of, d_of):
                    S.paired(ty, d)
                    S.sib_start(1 + ty, rem(b + d, SIDE))

        @pl.when(u == 18)
        def _():
            S.paired(0, 4)
            S.sib_start(1, rem(b + 4, SIDE))

        @pl.when(u < 5)
        def _():
            value_chunk(u)

        uh = u - 6 * c

        @pl.when(jnp.logical_and(uh >= 0, uh < 5))
        def _():
            halo_start(uh)

        @pl.when(jnp.logical_and(u >= 5, u < 10))
        def _():
            key_chunk(u - 5)

        @pl.when(jnp.logical_and(jnp.logical_and(uh >= 7, uh < 17), lax.rem(uh, 2) == 1))
        def _():
            halo_relay((uh - 7) // 2)

        @pl.when(jnp.logical_and(u >= 10, u < 12))
        def _():
            @pl.loop(0, 5)
            def _(k):
                state_group(5 * (u - 10) + k)

        pl.when(u == 11)(ar_a)
        pl.when(u == 13)(ar_b)
        pl.when(u == 18)(ar_c)
        pl.when(u == 23)(ar_d)
        pl.when(u == 16)(drain_first)

        @pl.when(u == 19)
        def _():
            S.sib_wait(1)

        @pl.when(u >= 19)
        def _():
            q_chunk(u - 19)

    @pl.loop(0, 4)
    def _(e):
        S.ring2q_last(1, e)
    ar_e()
    halo_finish()

    @pl.loop(0, 10)
    def _(g):
        conv_group(g)
    for d in (6, 2, 5, 3, 4):
        S.paired(1, d)
        S.sib_start(2, rem(b + d, SIDE))
    fin_copy(1 - c).wait_recv()
    for g in range(HD // 128):
        linear_group(g)
    S.sib_wait(2)

    @pl.loop(0, 8)
    def _(i):
        out_chunk(pl.multiple_of(i * 256, 256), 256)
    out_chunk(2048, 192)
    ar_drain()
    S.ring2_drain(1)
    S.sib_drain(1)
    S.sib_drain(2)


def body(tokens, shift, scale, gate, query_weight, pair_weight, output_weight, depth_taps):
    band, width, model = tokens.shape
    n = band * width
    dma = pltpu.SemaphoreType.DMA
    vm = pltpu.VMEM
    out, kvs = pl.pallas_call(
        kernel,
        out_shape=(jax.ShapeDtypeStruct((n, model), BF16), jax.ShapeDtypeStruct((HEADS, HEAD, HEAD), F32)),
        in_specs=[pl.BlockSpec(memory_space=vm)] * 8,
        out_specs=[pl.BlockSpec(memory_space=vm)] * 2,
        scratch_shapes=[
            vm((3, model), F32), vm((20, KP), BF16), vm((2, 10, KP), BF16),
            vm((SIDE, 4, UNIT, KP), BF16), vm((2, SIDE // 2, 2, 2, UNIT, KP), BF16),
            vm((4, 20, max(WIDTHS[0])), BF16), vm((8, 10, WMAX), BF16), vm((UNIT, WMAX), F32),
            dma((4,)), dma((4,)), dma((8,)), dma((8,)),
            dma((2, 7)), dma((2, 8)), dma((2, 2, 4, 8)), dma((2, 8, 8)), dma((3, 8)), dma((3, 8)), dma((2, 7, 8)),
            vm((n, KP), BF16), vm((n, HD), BF16), vm((n, HD), BF16), vm((band + 2, width, HD), F32),
            vm((n, HD), F32), vm((n, HD), BF16), vm((2, width, HD), BF16), vm((2, width, HD), BF16), vm((2, width, HD), BF16),
            vm((2, 192, 128), F32), vm((192, 128), F32), vm((SIDE, 24, 128), F32), vm((SIDE, 24, 128), F32),
            vm((24, 128), F32), vm((SIDE, 24, 128), F32), vm((24, 128), F32), vm((2, SIDE, 24, 128), F32),
            dma((2, 5)), dma((2, 5)), dma((2, 5)), dma((2, 5)), dma, dma, dma((8,)), dma((8,)), dma((8,)), dma((8,)), dma((8,)), dma((8,)), dma, dma,
        ],
        compiler_params=pltpu.CompilerParams(collective_id=0, has_side_effects=True, vmem_limit_bytes=50 << 20),
    )(
        tokens.reshape(n, model), shift, scale, gate, depth_taps,
        pair_weight.T, query_weight.T, output_weight,
    )
    return out.reshape(band, width, model), kvs


def solution(mesh):
    in_specs = (
        P(("clips", "rows"), None, None),
        P("clips"),
        P("clips"),
        P("clips"),
        P(None, "rows"),
        P(None, "rows"),
        P("rows", None),
        P(),
    )
    out_specs = (P(("clips", "rows"), None, None), P("clips", None, None))
    return jax.shard_map(body, mesh=mesh, in_specs=in_specs, out_specs=out_specs, check_vma=False)
```

```python
import jax
import jax.numpy as jnp
from jax import lax
from jax.experimental import pallas as pl
from jax.experimental.pallas import tpu as pltpu
from jax.sharding import PartitionSpec as P

HEADS, HEAD, FRAMES, HD = 40, 32, 8, 1280
NORM_EPS = 1e-06
DENOM_EPS = 1e-06
SIDE = 8
UNIT = 80
D = 2240
KP = 2304
WIDTHS = ((640, 512), (896, 256))
WMAX = 896
F32, BF16 = jnp.float32, jnp.bfloat16
NT = (((1,), (1,)), ((), ()))
TN = (((0,), (0,)), ((), ()))
NN = (((1,), (0,)), ((), ()))


def mm(lhs, rhs, dims):
    return lax.dot_general(lhs, rhs, dims, preferred_element_type=F32)


def rem(v, m):
    return lax.rem(v + m, m)


def gather_parts(kvsh, qosh, W0, W1, st_kv, st_qo, tmp, p0s, p0r, q0s, q0r, r1s, r1r, r2s, r2r, sbs, sbr, pzs):
    r = lax.axis_index("rows")
    c = lax.rem(r, 2)
    y = lax.rem(r // 2, SIDE)
    x = r // (2 * SIDE)
    j, p = y // 2, lax.rem(y, 2)
    i4 = y // 4
    a = jnp.where(c == 0, y, x)
    b = jnp.where(c == 0, x, y)
    wid = WIDTHS
    clip = lax.axis_index("clips")
    zp = lax.rem(clip, 2)
    pair = {"clips": clip + 1 - 2 * zp, "rows": r}

    def dev(xx, yy, cc):
        return {"rows": (xx * SIDE + yy) * 2 + cc}

    def at_ring(aa, bb):
        xx = jnp.where(c == 0, bb, aa)
        yy = jnp.where(c == 0, aa, bb)
        return dev(xx, yy, c)

    def by_core(fn):
        for cc in (0, 1):
            @pl.when(c == cc)
            def _(cc=cc):
                fn(cc)

    def coff(s, cc, pp):
        return pl.multiple_of(cc * 2 * wid[s][0] + pp * wid[s][cc], 128)

    def piece(cc, s, aa, bb):
        xx, yy = (bb, aa) if cc == 0 else (aa, bb)
        cols = pl.ds(coff(s, cc, lax.rem(yy, 2)), wid[s][cc])
        if s == 0:
            return W0.at[xx, yy // 2, :, cols]
        return W1.at[lax.rem(yy // 2 + xx, 2), xx // 2, lax.rem(xx, 2), yy // 4, :, cols]

    def barrier():
        sem = pltpu.get_barrier_semaphore()
        n = 0
        for m in range(1, 8):
            q = lax.rem(lax.rem(y, 4) * 2 + c + m, 8)
            pl.semaphore_signal(sem, inc=1, device_id=dev(x, 4 * i4 + q // 2, lax.rem(q, 2)))
            pl.semaphore_signal(sem, inc=1, device_id=dev(rem(x + m, SIDE), y, c))
            pl.semaphore_signal(sem, inc=1, device_id=dev(x, rem(y + m, SIDE), c))
            n += 3
        for k in (1, -1):
            pl.semaphore_signal(sem, inc=1, device_id=dev(rem(x + k, SIDE), rem(y + 2 * k, SIDE), c))
            n += 1
        pl.semaphore_signal(sem, inc=1, device_id=pair)
        pl.semaphore_wait(sem, n + 1)

    def rcopy(src, dst, ss, rs, d):
        return pltpu.make_async_remote_copy(src_ref=src, dst_ref=dst, send_sem=ss, recv_sem=rs, device_id=d,
                                            device_id_type=pl.DeviceIdType.MESH)

    def kv0(m):
        pd, cd = m // 2, m % 2
        w = wid[0][cd]
        src = kvsh.at[:, pl.ds(cd * 2 * wid[0][0] + pd * w, w)]
        slot = 2 * p + c
        dst = st_kv.at[slot, :, pl.ds(0, w)]
        return src, dst, slot, dev(x, 2 * j + pd, cd), (2 * p + c) == m

    def qo0(m):
        yd, cd = m // 2, m % 2
        pd, td = yd % 2, lax.rem(yd // 2 + x, 2)
        w = wid[1][cd]
        src = qosh.at[td, :, pl.ds(cd * 2 * wid[1][0] + pd * w, w)]
        slot = lax.rem(y, 4) * 2 + c
        dst = st_qo.at[slot, :, pl.ds(0, w)]
        return src, dst, slot, dev(x, 4 * i4 + yd, cd), slot == m

    def phase0_start(n, what, ss, rs):
        for m in range(n):
            src, dst, slot, d, own = what(m)

            @pl.when(own)
            def _():
                pltpu.make_async_copy(src, dst, rs.at[m]).start()

            @pl.when(jnp.logical_not(own))
            def _():
                rcopy(src, dst, ss.at[m], rs.at[slot], d).start()

    def phase0_wait(n, s, stage, rs):
        for m in range(n):
            def w(cc):
                ref = stage.at[m, :, pl.ds(0, wid[s][cc])]
                pltpu.make_async_copy(ref, ref, rs.at[m]).wait()
            by_core(w)

    def phase0_drain(n, what, ss, rs):
        for m in range(n):
            src, dst, slot, d, own = what(m)

            @pl.when(jnp.logical_not(own))
            def _():
                rcopy(src, dst, ss.at[m], rs.at[slot], d).wait_send()

    def build(s, n, stage):
        rows = UNIT // n
        for m in range(n):
            tmp[m * rows:(m + 1) * rows, 0:stage.shape[-1]] = stage[m].astype(jnp.float32)

        def put(cc):
            piece(cc, s, a, b)[...] = tmp[:, :wid[s][cc]].astype(jnp.bfloat16)
        by_core(put)

    def ap(e):
        d = (e + 1) // 2
        return rem(a + jnp.where(lax.rem(e, 2) == 1, -d, d), SIDE), d

    def r1copy(cc, s, k, aa, to):
        ref = piece(cc, s, aa, b)
        return rcopy(ref, ref, r1s.at[s, k], r1r.at[s, aa], at_ring(rem(a + to, SIDE), b))

    def ring1(s, e):
        aa, d = ap(e)

        @pl.when(e > 0)
        def _():
            by_core(lambda cc: r1copy(cc, s, 0, aa, 1).wait_recv())

        if s == 0:
            plan = ((0, 0, 1), (0, 1, -1), (0, 2, 2), (0, 3, -2), (3, 4, 1), (3, 5, 2), (4, 6, -1))
        else:
            plan = ((0, 0, 1), (0, 1, -1), (1, 2, 1), (2, 3, -1), (3, 4, 1), (4, 5, -1), (5, 6, 1))
        for when, k, to in plan:
            @pl.when(e == when)
            def _():
                by_core(lambda cc: r1copy(cc, s, k, aa, to).start())

    def ring1_drain(s):
        @pl.loop(0, 7)
        def _(k):
            by_core(lambda cc: r1copy(cc, s, k, a, 1).wait_send())

    def cp2(cc, s, dr, bb, aa, dl, e):
        ref = piece(cc, s, aa, bb)
        return rcopy(ref, ref, r2s.at[s, dr, dl, e], r2r.at[s, bb, aa], at_ring(a, rem(b + (1 if dr == 0 else SIDE - 1), SIDE)))

    def by_pair(s, typ, e, plane):
        if s == 0:
            return lax.rem(e, 4) == plane
        return e == lax.rem(typ + plane, 2)

    def onward(s, typ, dl, e, dr):
        low = e < (4 if s == 0 else 2)
        near = low if dr == 0 else jnp.logical_not(low)
        return jnp.logical_and(jnp.logical_not(by_pair(s, typ, e, zp)), jnp.logical_or(dl < 3, near))

    def zcopy(cc, s, aa, bb, k, e):
        ref = piece(cc, s, aa, bb)
        return rcopy(ref, ref, pzs.at[s, k, e], r2r.at[s, bb, aa], pair)

    def pick(s, typ, e, bb):
        if s == 0:
            return ap(e)[0]
        at_y = lax.rem(e, 2) + 4 * (e // 2) + 2 * lax.rem(typ + bb, 2)
        at_x = 2 * e + lax.rem(typ + bb // 2, 2)
        return jnp.where(c == 0, at_y, at_x)

    def step2(s, typ, dl, e, wait):
        e8 = 4 * typ + e
        for dr in (0, 1):
            bb = rem(b + (-dl if dr == 0 else dl), SIDE)
            aa = pick(s, typ, e, bb)
            if wait:
                @pl.when(jnp.logical_not(by_pair(s, typ, e, zp)))
                def _():
                    by_core(lambda cc: cp2(cc, s, dr, bb, aa, dl, e8).wait_recv())

            @pl.when(onward(s, typ, dl, e, dr))
            def _():
                by_core(lambda cc: cp2(cc, s, dr, bb, aa, dl, e8).start())
            if wait:
                @pl.when(by_pair(s, typ, e, 1 - zp))
                def _():
                    by_core(lambda cc: zcopy(cc, s, aa, bb, 2 * dl - 2 + dr, e8).start())

    def last2(s, typ, e):
        e8 = 4 * typ + e
        bb = rem(b + 4, SIDE)
        aa = pick(s, typ, e, bb)

        @pl.when(jnp.logical_not(by_pair(s, typ, e, zp)))
        def _():
            by_core(lambda cc: cp2(cc, s, 0, bb, aa, 3, e8).wait_recv())

        @pl.when(by_pair(s, typ, e, 1 - zp))
        def _():
            by_core(lambda cc: zcopy(cc, s, aa, bb, 6, e8).start())

    def paired(typ, d):
        bb = rem(b + d, SIDE)
        e = lax.rem(typ + zp, 2)
        aa = pick(1, typ, e, bb)
        by_core(lambda cc: cp2(cc, 1, 0, bb, aa, 3, 4 * typ + e).wait_recv())

    def paired0(d):
        bb = rem(b + d, SIDE)
        for k in (0, 4):
            e = k + zp
            aa = pick(0, 0, e, bb)
            by_core(lambda cc: cp2(cc, 0, 0, bb, aa, 3, e).wait_recv())

    def ring2(s, dl, e, wait):
        step2(0, 0, dl, e, wait)

    def ring2_last(s, e):
        last2(0, 0, e)

    def ring2q(typ, dl, e, wait):
        step2(1, typ, dl, e, wait)

    def ring2q_last(typ, e):
        last2(1, typ, e)

    def ring2_drain(s):
        @pl.loop(0, 32)
        def _(t):
            dl, e8 = t // 8, lax.rem(t, 8)
            e, typ = (e8, 0) if s == 0 else (lax.rem(e8, 4), e8 // 4)
            for dr in (0, 1):
                @pl.when(onward(s, typ, dl, e, dr))
                def _():
                    by_core(lambda cc: cp2(cc, s, dr, b, a, dl, e8).wait_send())

        @pl.loop(0, 14)
        def _(t):
            k, h = t // 2, lax.rem(t, 2)
            e8 = 4 * h + (1 - zp if s == 0 else lax.rem(h + 1 - zp, 2))
            by_core(lambda cc: zcopy(cc, s, a, b, k, e8).wait_send())

    def sib_ref(cc, s, bb):
        w = min(s, 1)
        if cc == 0:
            cols = pl.ds(0, 2 * wid[w][0])
            return W0.at[bb, :, :, cols] if s == 0 else W1.at[s - 1, bb // 2, lax.rem(bb, 2), :, :, cols]
        cols = pl.ds(coff(w, 1, lax.rem(bb, 2)), wid[w][1])
        if s == 0:
            return W0.at[:, bb // 2, :, cols]
        return W1.at[s - 1, :, lax.rem(s - 1 + bb // 2, 2), bb // 4, :, cols]

    def sib(cc, s, bb):
        ref = sib_ref(cc, s, bb)
        return rcopy(ref, ref, sbs.at[s, bb], sbr.at[s, bb], dev(x, y, 1 - c))

    def sib_start(s, bb):
        by_core(lambda cc: sib(cc, s, bb).start())

    def sib_wait(s):
        @pl.loop(0, SIDE)
        def _(bb):
            by_core(lambda cc: sib(1 - cc, s, bb).wait_recv())

    def sib_drain(s):
        @pl.loop(0, SIDE)
        def _(bb):
            by_core(lambda cc: sib(cc, s, bb).wait_send())

    ns = dict(locals())
    return ns


class Parts:
    pass


def kernel(tok, shift, scale, gate, taps, kvin, qin, oin, out, kvs,
           mod, kvsh, qosh,
           W0, W1, st_kv, st_qo, tmp, p0s, p0r, q0s, q0r, r1s, r1r, r2s, r2r, sbs, sbr, pzs,
           normed, keys, vals, vpad, local, mixed, hsend, hrecv, relay, pay, ara, red, rsx, part, agy, tot, fin,
           hs, hr, vs, vr, aas, aar, xs, xr, ys, yr, zs, zr, es, er):
    S = Parts()
    S.__dict__.update(gather_parts(kvsh, qosh, W0, W1, st_kv, st_qo, tmp, p0s, p0r, q0s, q0r, r1s, r1r,
                                   r2s, r2r, sbs, sbr, pzs))
    r, x, y, c, a, b = S.r, S.x, S.y, S.c, S.a, S.b
    total = 2 * SIDE * SIDE
    n_tok, width, band = 480, 120, 4
    kv_w = W0.reshape(2 * HD, KP)
    q_w = W1.at[0].reshape(HD, KP)
    o_w = W1.at[1].reshape(HD, KP)

    def norm(lo, hi):
        @pl.loop(lo, hi, unroll=2)
        def _(i):
            rows = pl.ds(pl.multiple_of(i * 16, 16), 16)
            v = tok[rows, :].astype(F32)
            center = v - jnp.mean(v, axis=-1, keepdims=True)
            spread = jnp.mean(center * center, axis=-1, keepdims=True)
            res = center * lax.rsqrt(spread + NORM_EPS) * (1.0 + mod[1:2, :]) + mod[0:1, :]
            normed[rows, 0:D] = res.astype(BF16)

    def lanes(i, n):
        return pl.ds(pl.multiple_of(i * n, n), n)

    def value_chunk(i):
        res = mm(normed[...], kv_w[pl.ds(pl.multiple_of(HD + i * 256, 256), 256), :], NT).astype(BF16)
        vals[:, lanes(i, 256)] = res
        wide = res.astype(F32)
        vpad[1:1 + band, :, lanes(i, 256)] = wide.reshape(band, width, 256)
        hsend[0, :, lanes(i, 256)] = wide[0:width].astype(BF16)
        hsend[1, :, lanes(i, 256)] = wide[n_tok - width:].astype(BF16)

    def key_chunk(i):
        res = mm(normed[...], kv_w[lanes(i, 256), :], NT)
        keys[:, lanes(i, 256)] = jnp.maximum(res, 0.0).astype(BF16)

    def q_chunk(i):
        res = mm(normed[...], q_w[lanes(i, 256), :], NT)
        keys[:, lanes(i, 256)] = jnp.maximum(res, 0.0).astype(BF16)

    def block_mask():
        i = lax.broadcasted_iota(jnp.int32, (128, 128), 0) // HEAD
        k = lax.broadcasted_iota(jnp.int32, (128, 128), 1) // HEAD
        return i == k

    def state_group(g):
        k = keys[:, lanes(g, 128)]
        s = mm(k, vals[:, lanes(g, 128)], TN)
        s = jnp.where(block_mask(), s, 0.0)
        s = s[0:32] + s[32:64] + s[64:96] + s[96:128]
        half, gg = g // 5, lax.rem(g, 5)
        pay[half, pl.ds(pl.multiple_of(gg * 32, 32), 32), :] = s
        ks = mm(jnp.ones((8, n_tok), BF16), k, NN)
        pay[half, pl.ds(160 + gg, 1), :] = ks[0:1]

    def halo(k, i):
        k2 = 2 if k else -2
        ln = lanes(i, 256)
        return S.rcopy(hsend.at[k, :, ln], relay.at[k, :, ln], hs.at[k, i], hr.at[k, i],
                       S.dev(x, rem(y + k2, SIDE), c))

    def hop(k, i):
        k2 = 2 if k else -2
        ln = lanes(i, 256)
        origin = S.dev(x, rem(y - k2, SIDE), c)["rows"]
        to = rem(origin + (FRAMES if k else total - FRAMES), total)
        has = origin < total - FRAMES if k else origin >= FRAMES
        return S.rcopy(relay.at[k, :, ln], hrecv.at[k, :, ln], vs.at[k, i], vr.at[k, i], {"rows": to}), has

    def sends(k):
        return r < total - FRAMES if k else r >= FRAMES

    def halo_start(i):
        for k in (0, 1):
            pl.when(sends(k))(lambda: halo(k, i).start())

    def halo_relay(i):
        for k in (0, 1):
            cp, has = hop(k, i)

            @pl.when(has)
            def _():
                halo(k, i).wait_recv()
                cp.start()

    def halo_finish():
        for k in (0, 1):
            row = band + 1 if k == 0 else 0

            @pl.when(sends(1 - k))
            def _():
                @pl.loop(0, 5)
                def _(i):
                    hop(k, i)[0].wait_recv()
                vpad[row] = hrecv[k].astype(F32)

            @pl.when(jnp.logical_not(sends(1 - k)))
            def _():
                vpad[row] = jnp.zeros((width, HD), F32)

    def halo_drain():
        @pl.loop(0, 5)
        def _(i):
            for k in (0, 1):
                pl.when(sends(k))(lambda: halo(k, i).wait_send())
                cp, has = hop(k, i)
                pl.when(has)(lambda: cp.wait_send())

    def conv_group(g):
        ln = lanes(g, 128)
        tp = taps[:, ln]
        col = lax.broadcasted_iota(jnp.int32, (width, 128), 0)
        acc = [None] * band
        for k in range(band + 2):
            v = vpad[k, :, ln]
            before = jnp.where(col == 0, 0.0, pltpu.roll(v, 1, 0))
            after = jnp.where(col == width - 1, 0.0, pltpu.roll(v, width - 1, 0))
            for o in range(band):
                m = k - o
                if 0 <= m <= 2:
                    term = tp[3 * m:3 * m + 1] * before + tp[3 * m + 1:3 * m + 2] * v + tp[3 * m + 2:3 * m + 3] * after
                    acc[o] = term if acc[o] is None else acc[o] + term
        for o in range(band):
            local[o * width:(o + 1) * width, ln] = acc[o]

    def arm():
        return S.rcopy(pay.at[1 - c], ara, aas, aar, S.dev(x, y, 1 - c))

    def ar_x(m):
        k = rem(a + m, SIDE)
        return S.rcopy(red.at[k], rsx.at[a], xs.at[k], xr.at[a], S.at_ring(k, b))

    def ar_y(m):
        k = rem(b + m, SIDE)
        return S.rcopy(part, agy.at[b], ys.at[k], yr.at[b], S.at_ring(a, k))

    def ar_z(m):
        k = rem(a + m, SIDE)
        return S.rcopy(tot, fin.at[c, a], zs.at[k], zr.at[a], S.at_ring(k, b))

    def arrived(m, buf, sem, me):
        k = rem(me + m, SIDE)
        pltpu.make_async_copy(buf.at[k], buf.at[k], sem.at[k]).wait()

    def sum8(buf):
        acc = buf[0]
        for k in range(1, SIDE):
            acc = acc + buf[k]
        return acc

    def ar_a():
        arm().start()

    def ar_b():
        arm().wait_recv()
        mine = pay[c] + ara[...]
        for k in range(SIDE):
            red[k] = mine[24 * k:24 * k + 24]
        rsx[a] = red[a]
        for m in range(1, SIDE):
            ar_x(m).start()

    def ar_c():
        for m in range(1, SIDE):
            arrived(m, rsx, xr, a)
        res = sum8(rsx)
        part[...] = res
        agy[b] = res
        for m in range(1, SIDE):
            ar_y(m).start()

    def ar_d():
        for m in range(1, SIDE):
            arrived(m, agy, yr, b)
        res = sum8(agy)
        tot[...] = res
        fin[c, a] = res
        for m in range(1, SIDE):
            ar_z(m).start()

    def fin_copy(h):
        return S.rcopy(fin.at[h], fin.at[h], es, er, S.dev(x, y, 1 - c))

    def ar_e():
        for m in range(1, SIDE):
            k = rem(a + m, SIDE)
            pltpu.make_async_copy(tot, tot, zr.at[k]).wait()
        fin_copy(c).start()

    def ar_drain():
        arm().wait_send()
        for m in range(1, SIDE):
            ar_x(m).wait_send()
            ar_y(m).wait_send()
            ar_z(m).wait_send()
        fin_copy(c).wait_send()
        halo_drain()

    def state_of(g):
        half, gg = g // 5, g % 5
        rows = []
        for k in range(4):
            at = 32 * gg + 8 * k
            rows.append(fin[half, at // 24, at % 24:at % 24 + 8])
        return jnp.concatenate(rows, axis=0), fin[half, 6, 16 + gg:17 + gg]

    def linear_group(g):
        s, ks = state_of(g)
        for h in range(4):
            kvs[4 * g + h] = s[:, 32 * h:32 * h + 32] / float(n_tok * total)
        mask = block_mask()
        bd = jnp.where(mask, jnp.concatenate([s] * 4, axis=0), 0.0)
        kd = jnp.where(mask, jnp.transpose(jnp.broadcast_to(ks, (128, 128))), 0.0)
        rhs = jnp.concatenate([bd, kd], axis=1)
        hi = rhs.astype(BF16)
        rest = rhs - hi.astype(F32)
        mid = rest.astype(BF16)
        lo = (rest - mid.astype(F32)).astype(BF16)
        q = keys[:, 128 * g:128 * g + 128]
        res = mm(q, hi, NN) + mm(q, mid, NN) + mm(q, lo, NN)
        lin = res[:, 0:128] / (res[:, 128:256] + DENOM_EPS)
        mixed[:, 128 * g:128 * g + 128] = (lin + local[:, 128 * g:128 * g + 128]).astype(BF16)

    def out_chunk(cols, n):
        w = o_w[:, pl.ds(cols, 256)]
        res = mm(mixed[...], w, NN)
        if n < 256:
            res = res[:, :n]
        ln = pl.ds(cols, n)
        out[:, ln] = (tok[:, ln].astype(F32) + mod[2:3, ln] * res).astype(BF16)

    def level(k, m):
        return jnp.where(k == 0, 0, 2 * k - 1 + m), jnp.logical_and(
            jnp.logical_and(k >= 0, k <= 4), jnp.logical_or(m == 0, jnp.logical_and(k >= 1, k <= 3)))

    def drain_first():
        S.phase0_drain(4, S.kv0, p0s, p0r)
        S.phase0_drain(8, S.qo0, q0s, q0r)
        S.ring1_drain(0)
        S.ring1_drain(1)
        S.ring2_drain(0)
        S.sib_drain(0)

    mod[0, :] = shift[...]
    mod[1, :] = scale[...]
    mod[2, :] = gate[...]
    kvsh[:, KP - 128:] = jnp.zeros((20, 128), BF16)
    qosh[:, :, KP - 128:] = jnp.zeros((2, 10, 128), BF16)
    kvsh[:, 0:D] = kvin[...]
    qosh[0, :, 0:D] = qin[...]
    qosh[1, :, 0:D] = oin[...]
    S.barrier()
    S.phase0_start(4, S.kv0, p0s, p0r)
    S.phase0_start(8, S.qo0, q0s, q0r)
    pay[0, 160:192, :] = jnp.zeros((32, 128), F32)
    pay[1, 160:192, :] = jnp.zeros((32, 128), F32)
    normed[:, KP - 128:] = jnp.zeros((n_tok, 128), BF16)
    norm(0, 20)
    S.phase0_wait(4, 0, st_kv, p0r)
    S.build(0, 4, st_kv)

    @pl.loop(0, 6)
    def _(diag):
        low, high = jnp.maximum(diag - 2, 0), jnp.minimum(diag, 3)

        @pl.loop(0, high - low + 1)
        def _(i):
            dl = high - i
            k = diag - dl
            first = jnp.where(k == 0, 0, jnp.where(k == 1, 1, 5))

            @pl.loop(0, jnp.where(k == 0, 1, jnp.where(k == 1, 4, 3)))
            def _(m):
                e = first + m

                @pl.when(dl == 0)
                def _():
                    S.ring1(0, e)
                    S.ring2(0, 0, e, False)

                @pl.when(dl > 0)
                def _():
                    S.ring2(0, dl, e, True)

        @pl.when(diag == 0)
        def _():
            norm(20, 30)

        @pl.when(diag == 1)
        def _():
            S.phase0_wait(8, 1, st_qo, q0r)
            S.build(1, 8, st_qo)
            S.ring1(1, jnp.int32(0))

        @pl.when(diag == 2)
        def _():
            S.sib_start(0, b)

        @pl.when(diag >= 3)
        def _():
            S.ring1(1, 2 * diag - 5)
            S.ring1(1, 2 * diag - 4)

        @pl.when(diag >= 4)
        def _():
            for d in (SIDE + 3 - diag, diag - 3):
                S.paired0(d)
                S.sib_start(0, rem(b + d, SIDE))

    S.ring1(1, jnp.int32(7))

    @pl.loop(0, 4)
    def _(e):
        S.ring2q(0, 0, e, False)

    @pl.loop(0, 8)
    def _(e):
        S.ring2_last(0, e)
    S.sib_start(1, b)
    S.sib_start(2, b)
    for d in (5, 3, 4):
        S.paired0(d)
        S.sib_start(0, rem(b + d, SIDE))
    S.sib_wait(0)

    @pl.loop(0, 24)
    def _(u):
        typ, dl, e = u // 12, 1 + lax.rem(u // 4, 3), lax.rem(u, 4)

        @pl.when(u == 8 - 3 * c)
        def _():
            @pl.loop(0, 4)
            def _(k):
                S.ring2q(1, 0, k, False)
        S.ring2q(typ, dl, e, True)

        @pl.when(jnp.logical_and(u >= 12, u < 16))
        def _():
            S.ring2q_last(0, e)

        for ty in (0, 1):
            group = u // 4 - 2
            d_of = 1 + lax.rem(rem(group, 6), 3)

            @pl.when(jnp.logical_and(jnp.logical_and(e == 1, group >= 0), (group >= 3) == (ty == 1)))
            def _():
                for d in (SIDE - d_of, d_of):
                    S.paired(ty, d)
                    S.sib_start(1 + ty, rem(b + d, SIDE))

        @pl.when(u == 18)
        def _():
            S.paired(0, 4)
            S.sib_start(1, rem(b + 4, SIDE))

        @pl.when(u < 5)
        def _():
            value_chunk(u)

        uh = u - 6 * c

        @pl.when(jnp.logical_and(uh >= 0, uh < 5))
        def _():
            halo_start(uh)

        @pl.when(jnp.logical_and(u >= 5, u < 10))
        def _():
            key_chunk(u - 5)

        @pl.when(jnp.logical_and(jnp.logical_and(uh >= 7, uh < 17), lax.rem(uh, 2) == 1))
        def _():
            halo_relay((uh - 7) // 2)

        @pl.when(jnp.logical_and(u >= 10, u < 12))
        def _():
            @pl.loop(0, 5)
            def _(k):
                state_group(5 * (u - 10) + k)

        pl.when(u == 11)(ar_a)
        pl.when(u == 13)(ar_b)
        pl.when(u == 18)(ar_c)
        pl.when(u == 23)(ar_d)
        pl.when(u == 16)(drain_first)

        @pl.when(u == 19)
        def _():
            S.sib_wait(1)

        @pl.when(u >= 19)
        def _():
            q_chunk(u - 19)

    @pl.loop(0, 4)
    def _(e):
        S.ring2q_last(1, e)
    ar_e()
    halo_finish()

    @pl.loop(0, 10)
    def _(g):
        conv_group(g)
    for d in (6, 2, 5, 3, 4):
        S.paired(1, d)
        S.sib_start(2, rem(b + d, SIDE))
    fin_copy(1 - c).wait_recv()
    for g in range(HD // 128):
        linear_group(g)
    S.sib_wait(2)

    @pl.loop(0, 8)
    def _(i):
        out_chunk(pl.multiple_of(i * 256, 256), 256)
    out_chunk(2048, 192)
    ar_drain()
    S.ring2_drain(1)
    S.sib_drain(1)
    S.sib_drain(2)


def body(tokens, shift, scale, gate, query_weight, pair_weight, output_weight, depth_taps):
    band, width, model = tokens.shape
    n = band * width
    dma = pltpu.SemaphoreType.DMA
    vm = pltpu.VMEM
    out, kvs = pl.pallas_call(
        kernel,
        out_shape=(jax.ShapeDtypeStruct((n, model), BF16), jax.ShapeDtypeStruct((HEADS, HEAD, HEAD), F32)),
        in_specs=[pl.BlockSpec(memory_space=vm)] * 8,
        out_specs=[pl.BlockSpec(memory_space=vm)] * 2,
        scratch_shapes=[
            vm((3, model), F32), vm((20, KP), BF16), vm((2, 10, KP), BF16),
            vm((SIDE, 4, UNIT, KP), BF16), vm((2, SIDE // 2, 2, 2, UNIT, KP), BF16),
            vm((4, 20, max(WIDTHS[0])), BF16), vm((8, 10, WMAX), BF16), vm((UNIT, WMAX), F32),
            dma((4,)), dma((4,)), dma((8,)), dma((8,)),
            dma((2, 7)), dma((2, 8)), dma((2, 2, 4, 8)), dma((2, 8, 8)), dma((3, 8)), dma((3, 8)), dma((2, 7, 8)),
            vm((n, KP), BF16), vm((n, HD), BF16), vm((n, HD), BF16), vm((band + 2, width, HD), F32),
            vm((n, HD), F32), vm((n, HD), BF16), vm((2, width, HD), BF16), vm((2, width, HD), BF16), vm((2, width, HD), BF16),
            vm((2, 192, 128), F32), vm((192, 128), F32), vm((SIDE, 24, 128), F32), vm((SIDE, 24, 128), F32),
            vm((24, 128), F32), vm((SIDE, 24, 128), F32), vm((24, 128), F32), vm((2, SIDE, 24, 128), F32),
            dma((2, 5)), dma((2, 5)), dma((2, 5)), dma((2, 5)), dma, dma, dma((8,)), dma((8,)), dma((8,)), dma((8,)), dma((8,)), dma((8,)), dma, dma,
        ],
        compiler_params=pltpu.CompilerParams(collective_id=0, has_side_effects=True, vmem_limit_bytes=50 << 20),
    )(
        tokens.reshape(n, model), shift, scale, gate, depth_taps,
        pair_weight.T, query_weight.T, output_weight,
    )
    return out.reshape(band, width, model), kvs


def solution(mesh):
    in_specs = (
        P(("clips", "rows"), None, None),
        P("clips"),
        P("clips"),
        P("clips"),
        P(None, "rows"),
        P(None, "rows"),
        P("rows", None),
        P(),
    )
    out_specs = (P(("clips", "rows"), None, None), P("clips", None, None))
    return jax.shard_map(body, mesh=mesh, in_specs=in_specs, out_specs=out_specs, check_vma=False)
```

```python
import jax
import jax.numpy as jnp
from jax import lax
from jax.experimental import pallas as pl
from jax.experimental.pallas import tpu as pltpu
from jax.sharding import PartitionSpec as P

HEADS, HEAD, FRAMES, HD = 40, 32, 8, 1280
NORM_EPS = 1e-06
DENOM_EPS = 1e-06
SIDE = 8
UNIT = 80
D = 2240
KP = 2304
WIDTHS = ((640, 512), (896, 256))
WMAX = 896
F32, BF16 = jnp.float32, jnp.bfloat16
NT = (((1,), (1,)), ((), ()))
TN = (((0,), (0,)), ((), ()))
NN = (((1,), (0,)), ((), ()))


def mm(lhs, rhs, dims):
    return lax.dot_general(lhs, rhs, dims, preferred_element_type=F32)


def rem(v, m):
    return lax.rem(v + m, m)


def gather_parts(kvsh, qosh, W0, W1, st_kv, st_qo, tmp, p0s, p0r, q0s, q0r, r1s, r1r, r2s, r2r, sbs, sbr, pzs):
    r = lax.axis_index("rows")
    c = lax.rem(r, 2)
    y = lax.rem(r // 2, SIDE)
    x = r // (2 * SIDE)
    j, p = y // 2, lax.rem(y, 2)
    i4 = y // 4
    a = jnp.where(c == 0, y, x)
    b = jnp.where(c == 0, x, y)
    wid = WIDTHS
    clip = lax.axis_index("clips")
    zp = lax.rem(clip, 2)
    pair = {"clips": clip + 1 - 2 * zp, "rows": r}

    def dev(xx, yy, cc):
        return {"rows": (xx * SIDE + yy) * 2 + cc}

    def at_ring(aa, bb):
        xx = jnp.where(c == 0, bb, aa)
        yy = jnp.where(c == 0, aa, bb)
        return dev(xx, yy, c)

    def by_core(fn):
        for cc in (0, 1):
            @pl.when(c == cc)
            def _(cc=cc):
                fn(cc)

    def coff(s, cc, pp):
        return pl.multiple_of(cc * 2 * wid[s][0] + pp * wid[s][cc], 128)

    def piece(cc, s, aa, bb):
        xx, yy = (bb, aa) if cc == 0 else (aa, bb)
        cols = pl.ds(coff(s, cc, lax.rem(yy, 2)), wid[s][cc])
        if s == 0:
            return W0.at[xx, yy // 2, :, cols]
        return W1.at[lax.rem(yy // 2 + xx, 2), xx // 2, lax.rem(xx, 2), yy // 4, :, cols]

    def barrier():
        sem = pltpu.get_barrier_semaphore()
        n = 0
        for m in range(1, 8):
            q = lax.rem(lax.rem(y, 4) * 2 + c + m, 8)
            pl.semaphore_signal(sem, inc=1, device_id=dev(x, 4 * i4 + q // 2, lax.rem(q, 2)))
            pl.semaphore_signal(sem, inc=1, device_id=dev(rem(x + m, SIDE), y, c))
            pl.semaphore_signal(sem, inc=1, device_id=dev(x, rem(y + m, SIDE), c))
            n += 3
        for k in (1, -1):
            pl.semaphore_signal(sem, inc=1, device_id=dev(rem(x + k, SIDE), rem(y + 2 * k, SIDE), c))
            n += 1
        pl.semaphore_signal(sem, inc=1, device_id=pair)
        pl.semaphore_wait(sem, n + 1)

    def rcopy(src, dst, ss, rs, d):
        return pltpu.make_async_remote_copy(src_ref=src, dst_ref=dst, send_sem=ss, recv_sem=rs, device_id=d,
                                            device_id_type=pl.DeviceIdType.MESH)

    def kv0(m):
        pd, cd = m // 2, m % 2
        w = wid[0][cd]
        src = kvsh.at[:, pl.ds(cd * 2 * wid[0][0] + pd * w, w)]
        slot = 2 * p + c
        dst = st_kv.at[slot, :, pl.ds(0, w)]
        return src, dst, slot, dev(x, 2 * j + pd, cd), (2 * p + c) == m

    def qo0(m):
        yd, cd = m // 2, m % 2
        pd, td = yd % 2, lax.rem(yd // 2 + x, 2)
        w = wid[1][cd]
        src = qosh.at[td, :, pl.ds(cd * 2 * wid[1][0] + pd * w, w)]
        slot = lax.rem(y, 4) * 2 + c
        dst = st_qo.at[slot, :, pl.ds(0, w)]
        return src, dst, slot, dev(x, 4 * i4 + yd, cd), slot == m

    def phase0_start(n, what, ss, rs):
        for m in range(n):
            src, dst, slot, d, own = what(m)

            @pl.when(own)
            def _():
                pltpu.make_async_copy(src, dst, rs.at[m]).start()

            @pl.when(jnp.logical_not(own))
            def _():
                rcopy(src, dst, ss.at[m], rs.at[slot], d).start()

    def phase0_wait(n, s, stage, rs):
        for m in range(n):
            def w(cc):
                ref = stage.at[m, :, pl.ds(0, wid[s][cc])]
                pltpu.make_async_copy(ref, ref, rs.at[m]).wait()
            by_core(w)

    def phase0_drain(n, what, ss, rs):
        for m in range(n):
            src, dst, slot, d, own = what(m)

            @pl.when(jnp.logical_not(own))
            def _():
                rcopy(src, dst, ss.at[m], rs.at[slot], d).wait_send()

    def build(s, n, stage):
        rows = UNIT // n
        for m in range(n):
            tmp[m * rows:(m + 1) * rows, 0:stage.shape[-1]] = stage[m].astype(jnp.float32)

        def put(cc):
            piece(cc, s, a, b)[...] = tmp[:, :wid[s][cc]].astype(jnp.bfloat16)
        by_core(put)

    def ap(e):
        d = (e + 1) // 2
        return rem(a + jnp.where(lax.rem(e, 2) == 1, -d, d), SIDE), d

    def r1copy(cc, s, k, aa, to):
        ref = piece(cc, s, aa, b)
        return rcopy(ref, ref, r1s.at[s, k], r1r.at[s, aa], at_ring(rem(a + to, SIDE), b))

    def ring1(s, e):
        aa, d = ap(e)

        @pl.when(e > 0)
        def _():
            by_core(lambda cc: r1copy(cc, s, 0, aa, 1).wait_recv())

        if s == 0:
            plan = ((0, 0, 1), (0, 1, -1), (0, 2, 2), (0, 3, -2), (3, 4, 1), (3, 5, 2), (4, 6, -1))
        else:
            plan = ((0, 0, 1), (0, 1, -1), (1, 2, 1), (2, 3, -1), (3, 4, 1), (4, 5, -1), (5, 6, 1))
        for when, k, to in plan:
            @pl.when(e == when)
            def _():
                by_core(lambda cc: r1copy(cc, s, k, aa, to).start())

    def ring1_drain(s):
        @pl.loop(0, 7)
        def _(k):
            by_core(lambda cc: r1copy(cc, s, k, a, 1).wait_send())

    def cp2(cc, s, dr, bb, aa, dl, e):
        ref = piece(cc, s, aa, bb)
        return rcopy(ref, ref, r2s.at[s, dr, dl, e], r2r.at[s, bb, aa], at_ring(a, rem(b + (1 if dr == 0 else SIDE - 1), SIDE)))

    def by_pair(s, typ, e, plane):
        if s == 0:
            return lax.rem(e, 4) == plane
        return e == lax.rem(typ + plane, 2)

    def onward(s, typ, dl, e, dr):
        low = e < (4 if s == 0 else 2)
        near = low if dr == 0 else jnp.logical_not(low)
        return jnp.logical_and(jnp.logical_not(by_pair(s, typ, e, zp)), jnp.logical_or(dl < 3, near))

    def zcopy(cc, s, aa, bb, k, e):
        ref = piece(cc, s, aa, bb)
        return rcopy(ref, ref, pzs.at[s, k, e], r2r.at[s, bb, aa], pair)

    def pick(s, typ, e, bb):
        if s == 0:
            return ap(e)[0]
        at_y = lax.rem(e, 2) + 4 * (e // 2) + 2 * lax.rem(typ + bb, 2)
        at_x = 2 * e + lax.rem(typ + bb // 2, 2)
        return jnp.where(c == 0, at_y, at_x)

    def step2(s, typ, dl, e, wait):
        e8 = 4 * typ + e
        for dr in (0, 1):
            bb = rem(b + (-dl if dr == 0 else dl), SIDE)
            aa = pick(s, typ, e, bb)
            if wait:
                @pl.when(jnp.logical_not(by_pair(s, typ, e, zp)))
                def _():
                    by_core(lambda cc: cp2(cc, s, dr, bb, aa, dl, e8).wait_recv())

            @pl.when(onward(s, typ, dl, e, dr))
            def _():
                by_core(lambda cc: cp2(cc, s, dr, bb, aa, dl, e8).start())
            if wait:
                @pl.when(by_pair(s, typ, e, 1 - zp))
                def _():
                    by_core(lambda cc: zcopy(cc, s, aa, bb, 2 * dl - 2 + dr, e8).start())

    def last2(s, typ, e):
        e8 = 4 * typ + e
        bb = rem(b + 4, SIDE)
        aa = pick(s, typ, e, bb)

        @pl.when(jnp.logical_not(by_pair(s, typ, e, zp)))
        def _():
            by_core(lambda cc: cp2(cc, s, 0, bb, aa, 3, e8).wait_recv())

        @pl.when(by_pair(s, typ, e, 1 - zp))
        def _():
            by_core(lambda cc: zcopy(cc, s, aa, bb, 6, e8).start())

    def paired(typ, d):
        bb = rem(b + d, SIDE)
        e = lax.rem(typ + zp, 2)
        aa = pick(1, typ, e, bb)
        by_core(lambda cc: cp2(cc, 1, 0, bb, aa, 3, 4 * typ + e).wait_recv())

    def paired0(d):
        bb = rem(b + d, SIDE)
        for k in (0, 4):
            e = k + zp
            aa = pick(0, 0, e, bb)
            by_core(lambda cc: cp2(cc, 0, 0, bb, aa, 3, e).wait_recv())

    def ring2(s, dl, e, wait):
        step2(0, 0, dl, e, wait)

    def ring2_last(s, e):
        last2(0, 0, e)

    def ring2q(typ, dl, e, wait):
        step2(1, typ, dl, e, wait)

    def ring2q_last(typ, e):
        last2(1, typ, e)

    def ring2_drain(s):
        @pl.loop(0, 32)
        def _(t):
            dl, e8 = t // 8, lax.rem(t, 8)
            e, typ = (e8, 0) if s == 0 else (lax.rem(e8, 4), e8 // 4)
            for dr in (0, 1):
                @pl.when(onward(s, typ, dl, e, dr))
                def _():
                    by_core(lambda cc: cp2(cc, s, dr, b, a, dl, e8).wait_send())

        @pl.loop(0, 14)
        def _(t):
            k, h = t // 2, lax.rem(t, 2)
            e8 = 4 * h + (1 - zp if s == 0 else lax.rem(h + 1 - zp, 2))
            by_core(lambda cc: zcopy(cc, s, a, b, k, e8).wait_send())

    def sib_ref(cc, s, bb):
        w = min(s, 1)
        if cc == 0:
            cols = pl.ds(0, 2 * wid[w][0])
            return W0.at[bb, :, :, cols] if s == 0 else W1.at[s - 1, bb // 2, lax.rem(bb, 2), :, :, cols]
        cols = pl.ds(coff(w, 1, lax.rem(bb, 2)), wid[w][1])
        if s == 0:
            return W0.at[:, bb // 2, :, cols]
        return W1.at[s - 1, :, lax.rem(s - 1 + bb // 2, 2), bb // 4, :, cols]

    def sib(cc, s, bb):
        ref = sib_ref(cc, s, bb)
        return rcopy(ref, ref, sbs.at[s, bb], sbr.at[s, bb], dev(x, y, 1 - c))

    def sib_start(s, bb):
        by_core(lambda cc: sib(cc, s, bb).start())

    def sib_wait(s):
        @pl.loop(0, SIDE)
        def _(bb):
            by_core(lambda cc: sib(1 - cc, s, bb).wait_recv())

    def sib_drain(s):
        @pl.loop(0, SIDE)
        def _(bb):
            by_core(lambda cc: sib(cc, s, bb).wait_send())

    ns = dict(locals())
    return ns


class Parts:
    pass


def kernel(tok, shift, scale, gate, taps, kvin, qin, oin, out, kvs,
           mod, kvsh, qosh,
           W0, W1, st_kv, st_qo, tmp, p0s, p0r, q0s, q0r, r1s, r1r, r2s, r2r, sbs, sbr, pzs,
           normed, keys, vals, vpad, local, mixed, hsend, hrecv, relay, pay, ara, red, rsx, part, agy, tot, fin,
           hs, hr, vs, vr, aas, aar, xs, xr, ys, yr, zs, zr, es, er):
    S = Parts()
    S.__dict__.update(gather_parts(kvsh, qosh, W0, W1, st_kv, st_qo, tmp, p0s, p0r, q0s, q0r, r1s, r1r,
                                   r2s, r2r, sbs, sbr, pzs))
    r, x, y, c, a, b = S.r, S.x, S.y, S.c, S.a, S.b
    total = 2 * SIDE * SIDE
    n_tok, width, band = 480, 120, 4
    kv_w = W0.reshape(2 * HD, KP)
    q_w = W1.at[0].reshape(HD, KP)
    o_w = W1.at[1].reshape(HD, KP)

    def norm(lo, hi):
        @pl.loop(lo, hi, unroll=2)
        def _(i):
            rows = pl.ds(pl.multiple_of(i * 16, 16), 16)
            v = tok[rows, :].astype(F32)
            center = v - jnp.mean(v, axis=-1, keepdims=True)
            spread = jnp.mean(center * center, axis=-1, keepdims=True)
            res = center * lax.rsqrt(spread + NORM_EPS) * (1.0 + mod[1:2, :]) + mod[0:1, :]
            normed[rows, 0:D] = res.astype(BF16)

    def lanes(i, n):
        return pl.ds(pl.multiple_of(i * n, n), n)

    def value_chunk(i):
        res = mm(normed[...], kv_w[pl.ds(pl.multiple_of(HD + i * 256, 256), 256), :], NT).astype(BF16)
        vals[:, lanes(i, 256)] = res
        wide = res.astype(F32)
        vpad[1:1 + band, :, lanes(i, 256)] = wide.reshape(band, width, 256)
        hsend[0, :, lanes(i, 256)] = wide[0:width].astype(BF16)
        hsend[1, :, lanes(i, 256)] = wide[n_tok - width:].astype(BF16)

    def key_chunk(i):
        res = mm(normed[...], kv_w[lanes(i, 256), :], NT)
        keys[:, lanes(i, 256)] = jnp.maximum(res, 0.0).astype(BF16)

    def q_chunk(i):
        res = mm(normed[...], q_w[lanes(i, 256), :], NT)
        keys[:, lanes(i, 256)] = jnp.maximum(res, 0.0).astype(BF16)

    def block_mask():
        i = lax.broadcasted_iota(jnp.int32, (128, 128), 0) // HEAD
        k = lax.broadcasted_iota(jnp.int32, (128, 128), 1) // HEAD
        return i == k

    def state_group(g):
        k = keys[:, lanes(g, 128)]
        s = mm(k, vals[:, lanes(g, 128)], TN)
        s = jnp.where(block_mask(), s, 0.0)
        s = s[0:32] + s[32:64] + s[64:96] + s[96:128]
        half, gg = g // 5, lax.rem(g, 5)
        pay[half, pl.ds(pl.multiple_of(gg * 32, 32), 32), :] = s
        ks = mm(jnp.ones((8, n_tok), BF16), k, NN)
        pay[half, pl.ds(160 + gg, 1), :] = ks[0:1]

    def halo(k, i):
        k2 = 2 if k else -2
        ln = lanes(i, 256)
        return S.rcopy(hsend.at[k, :, ln], relay.at[k, :, ln], hs.at[k, i], hr.at[k, i],
                       S.dev(x, rem(y + k2, SIDE), c))

    def hop(k, i):
        k2 = 2 if k else -2
        ln = lanes(i, 256)
        origin = S.dev(x, rem(y - k2, SIDE), c)["rows"]
        to = rem(origin + (FRAMES if k else total - FRAMES), total)
        has = origin < total - FRAMES if k else origin >= FRAMES
        return S.rcopy(relay.at[k, :, ln], hrecv.at[k, :, ln], vs.at[k, i], vr.at[k, i], {"rows": to}), has

    def sends(k):
        return r < total - FRAMES if k else r >= FRAMES

    def halo_start(i):
        for k in (0, 1):
            pl.when(sends(k))(lambda: halo(k, i).start())

    def halo_relay(i):
        for k in (0, 1):
            cp, has = hop(k, i)

            @pl.when(has)
            def _():
                halo(k, i).wait_recv()
                cp.start()

    def halo_finish():
        for k in (0, 1):
            row = band + 1 if k == 0 else 0

            @pl.when(sends(1 - k))
            def _():
                @pl.loop(0, 5)
                def _(i):
                    hop(k, i)[0].wait_recv()
                vpad[row] = hrecv[k].astype(F32)

            @pl.when(jnp.logical_not(sends(1 - k)))
            def _():
                vpad[row] = jnp.zeros((width, HD), F32)

    def halo_drain():
        @pl.loop(0, 5)
        def _(i):
            for k in (0, 1):
                pl.when(sends(k))(lambda: halo(k, i).wait_send())
                cp, has = hop(k, i)
                pl.when(has)(lambda: cp.wait_send())

    def conv_group(g):
        ln = lanes(g, 128)
        tp = taps[:, ln]
        col = lax.broadcasted_iota(jnp.int32, (width, 128), 0)
        acc = [None] * band
        for k in range(band + 2):
            v = vpad[k, :, ln]
            before = jnp.where(col == 0, 0.0, pltpu.roll(v, 1, 0))
            after = jnp.where(col == width - 1, 0.0, pltpu.roll(v, width - 1, 0))
            for o in range(band):
                m = k - o
                if 0 <= m <= 2:
                    term = tp[3 * m:3 * m + 1] * before + tp[3 * m + 1:3 * m + 2] * v + tp[3 * m + 2:3 * m + 3] * after
                    acc[o] = term if acc[o] is None else acc[o] + term
        for o in range(band):
            local[o * width:(o + 1) * width, ln] = acc[o]

    def arm():
        return S.rcopy(pay.at[1 - c], ara, aas, aar, S.dev(x, y, 1 - c))

    def ar_x(m):
        k = rem(a + m, SIDE)
        return S.rcopy(red.at[k], rsx.at[a], xs.at[k], xr.at[a], S.at_ring(k, b))

    def ar_y(m):
        k = rem(b + m, SIDE)
        return S.rcopy(part, agy.at[b], ys.at[k], yr.at[b], S.at_ring(a, k))

    def ar_z(m):
        k = rem(a + m, SIDE)
        return S.rcopy(tot, fin.at[c, a], zs.at[k], zr.at[a], S.at_ring(k, b))

    def arrived(m, buf, sem, me):
        k = rem(me + m, SIDE)
        pltpu.make_async_copy(buf.at[k], buf.at[k], sem.at[k]).wait()

    def sum8(buf):
        acc = buf[0]
        for k in range(1, SIDE):
            acc = acc + buf[k]
        return acc

    def ar_a():
        arm().start()

    def ar_b():
        arm().wait_recv()
        mine = pay[c] + ara[...]
        for k in range(SIDE):
            red[k] = mine[24 * k:24 * k + 24]
        rsx[a] = red[a]
        for m in range(1, SIDE):
            ar_x(m).start()

    def ar_c():
        for m in range(1, SIDE):
            arrived(m, rsx, xr, a)
        res = sum8(rsx)
        part[...] = res
        agy[b] = res
        for m in range(1, SIDE):
            ar_y(m).start()

    def ar_d():
        for m in range(1, SIDE):
            arrived(m, agy, yr, b)
        res = sum8(agy)
        tot[...] = res
        fin[c, a] = res
        for m in range(1, SIDE):
            ar_z(m).start()

    def fin_copy(h):
        return S.rcopy(fin.at[h], fin.at[h], es, er, S.dev(x, y, 1 - c))

    def ar_e():
        for m in range(1, SIDE):
            k = rem(a + m, SIDE)
            pltpu.make_async_copy(tot, tot, zr.at[k]).wait()
        fin_copy(c).start()

    def ar_drain():
        arm().wait_send()
        for m in range(1, SIDE):
            ar_x(m).wait_send()
            ar_y(m).wait_send()
            ar_z(m).wait_send()
        fin_copy(c).wait_send()
        halo_drain()

    def state_of(g):
        half, gg = g // 5, g % 5
        rows = []
        for k in range(4):
            at = 32 * gg + 8 * k
            rows.append(fin[half, at // 24, at % 24:at % 24 + 8])
        return jnp.concatenate(rows, axis=0), fin[half, 6, 16 + gg:17 + gg]

    def linear_group(g):
        s, ks = state_of(g)
        for h in range(4):
            kvs[4 * g + h] = s[:, 32 * h:32 * h + 32] / float(n_tok * total)
        mask = block_mask()
        bd = jnp.where(mask, jnp.concatenate([s] * 4, axis=0), 0.0)
        kd = jnp.where(mask, jnp.transpose(jnp.broadcast_to(ks, (128, 128))), 0.0)
        rhs = jnp.concatenate([bd, kd], axis=1)
        hi = rhs.astype(BF16)
        rest = rhs - hi.astype(F32)
        mid = rest.astype(BF16)
        lo = (rest - mid.astype(F32)).astype(BF16)
        q = keys[:, 128 * g:128 * g + 128]
        res = mm(q, hi, NN) + mm(q, mid, NN) + mm(q, lo, NN)
        lin = res[:, 0:128] / (res[:, 128:256] + DENOM_EPS)
        mixed[:, 128 * g:128 * g + 128] = (lin + local[:, 128 * g:128 * g + 128]).astype(BF16)

    def out_chunk(cols, n):
        w = o_w[:, pl.ds(cols, 256)]
        res = mm(mixed[...], w, NN)
        if n < 256:
            res = res[:, :n]
        ln = pl.ds(cols, n)
        out[:, ln] = (tok[:, ln].astype(F32) + mod[2:3, ln] * res).astype(BF16)

    def level(k, m):
        return jnp.where(k == 0, 0, 2 * k - 1 + m), jnp.logical_and(
            jnp.logical_and(k >= 0, k <= 4), jnp.logical_or(m == 0, jnp.logical_and(k >= 1, k <= 3)))

    def drain_first():
        S.phase0_drain(4, S.kv0, p0s, p0r)
        S.phase0_drain(8, S.qo0, q0s, q0r)
        S.ring1_drain(0)
        S.ring1_drain(1)
        S.ring2_drain(0)
        S.sib_drain(0)

    def convolve():
        halo_finish()

        @pl.loop(0, HD // 128)
        def _(g):
            conv_group(g)

    mod[0, :] = shift[...]
    mod[1, :] = scale[...]
    mod[2, :] = gate[...]
    kvsh[:, KP - 128:] = jnp.zeros((20, 128), BF16)
    qosh[:, :, KP - 128:] = jnp.zeros((2, 10, 128), BF16)
    kvsh[:, 0:D] = kvin[...]
    qosh[0, :, 0:D] = qin[...]
    qosh[1, :, 0:D] = oin[...]
    S.barrier()
    S.phase0_start(4, S.kv0, p0s, p0r)
    S.phase0_start(8, S.qo0, q0s, q0r)
    pay[0, 160:192, :] = jnp.zeros((32, 128), F32)
    pay[1, 160:192, :] = jnp.zeros((32, 128), F32)
    normed[:, KP - 128:] = jnp.zeros((n_tok, 128), BF16)
    norm(0, 20)
    S.phase0_wait(4, 0, st_kv, p0r)
    S.build(0, 4, st_kv)

    @pl.loop(0, 6)
    def _(diag):
        low, high = jnp.maximum(diag - 2, 0), jnp.minimum(diag, 3)

        @pl.loop(0, high - low + 1)
        def _(i):
            dl = high - i
            k = diag - dl
            first = jnp.where(k == 0, 0, jnp.where(k == 1, 1, 5))

            @pl.loop(0, jnp.where(k == 0, 1, jnp.where(k == 1, 4, 3)))
            def _(m):
                e = first + m

                @pl.when(dl == 0)
                def _():
                    S.ring1(0, e)
                    S.ring2(0, 0, e, False)

                @pl.when(dl > 0)
                def _():
                    S.ring2(0, dl, e, True)

        @pl.when(diag == 0)
        def _():
            norm(20, 30)

        @pl.when(diag == 1)
        def _():
            S.phase0_wait(8, 1, st_qo, q0r)
            S.build(1, 8, st_qo)
            S.ring1(1, jnp.int32(0))

        @pl.when(diag == 2)
        def _():
            S.sib_start(0, b)

        @pl.when(diag >= 3)
        def _():
            S.ring1(1, 2 * diag - 5)
            S.ring1(1, 2 * diag - 4)

        @pl.when(diag >= 4)
        def _():
            for d in (SIDE + 3 - diag, diag - 3):
                S.paired0(d)
                S.sib_start(0, rem(b + d, SIDE))

    S.ring1(1, jnp.int32(7))

    @pl.loop(0, 4)
    def _(e):
        S.ring2q(0, 0, e, False)

    @pl.loop(0, 8)
    def _(e):
        S.ring2_last(0, e)
    S.sib_start(1, b)
    S.sib_start(2, b)
    for d in (5, 3, 4):
        S.paired0(d)
        S.sib_start(0, rem(b + d, SIDE))
    S.sib_wait(0)

    @pl.loop(0, 24)
    def _(u):
        typ, dl, e = u // 12, 1 + lax.rem(u // 4, 3), lax.rem(u, 4)

        @pl.when(u == 8 - 3 * c)
        def _():
            @pl.loop(0, 4)
            def _(k):
                S.ring2q(1, 0, k, False)
        S.ring2q(typ, dl, e, True)

        @pl.when(jnp.logical_and(u >= 12, u < 16))
        def _():
            S.ring2q_last(0, e)

        for ty in (0, 1):
            group = u // 4 - 2
            d_of = 1 + lax.rem(rem(group, 6), 3)

            @pl.when(jnp.logical_and(jnp.logical_and(e == 1, group >= 0), (group >= 3) == (ty == 1)))
            def _():
                for d in (SIDE - d_of, d_of):
                    S.paired(ty, d)
                    S.sib_start(1 + ty, rem(b + d, SIDE))

        @pl.when(u == 18)
        def _():
            S.paired(0, 4)
            S.sib_start(1, rem(b + 4, SIDE))

        @pl.when(u < 5)
        def _():
            value_chunk(u)

        uh = u - 6 * c

        @pl.when(jnp.logical_and(uh >= 0, uh < 5))
        def _():
            halo_start(uh)

        @pl.when(jnp.logical_and(u >= 5, u < 10))
        def _():
            key_chunk(u - 5)

        @pl.when(jnp.logical_and(jnp.logical_and(uh >= 7, uh < 17), lax.rem(uh, 2) == 1))
        def _():
            halo_relay((uh - 7) // 2)

        @pl.when(jnp.logical_and(u >= 10, u < 12))
        def _():
            @pl.loop(0, 5)
            def _(k):
                state_group(5 * (u - 10) + k)

        pl.when(u == 11)(ar_a)
        pl.when(u == 13)(ar_b)
        pl.when(u == 18)(ar_c)
        pl.when(u == 23)(ar_d)
        pl.when(u == 16)(drain_first)

        @pl.when(u == 19)
        def _():
            S.sib_wait(1)

        @pl.when(u >= 19)
        def _():
            q_chunk(u - 19)

        pl.when(jnp.logical_and(u == 21, c == 0))(convolve)

    @pl.loop(0, 4)
    def _(e):
        S.ring2q_last(1, e)
    ar_e()
    pl.when(c == 1)(convolve)
    for d in (6, 2, 5, 3, 4):
        S.paired(1, d)
        S.sib_start(2, rem(b + d, SIDE))
    fin_copy(1 - c).wait_recv()
    for g in range(HD // 128):
        linear_group(g)
    ar_drain()
    S.ring2_drain(1)
    S.sib_drain(1)
    S.sib_wait(2)

    @pl.loop(0, 8)
    def _(i):
        out_chunk(pl.multiple_of(i * 256, 256), 256)
    out_chunk(2048, 192)
    S.sib_drain(2)


def body(tokens, shift, scale, gate, query_weight, pair_weight, output_weight, depth_taps):
    band, width, model = tokens.shape
    n = band * width
    dma = pltpu.SemaphoreType.DMA
    vm = pltpu.VMEM
    out, kvs = pl.pallas_call(
        kernel,
        out_shape=(jax.ShapeDtypeStruct((n, model), BF16), jax.ShapeDtypeStruct((HEADS, HEAD, HEAD), F32)),
        in_specs=[pl.BlockSpec(memory_space=vm)] * 8,
        out_specs=[pl.BlockSpec(memory_space=vm)] * 2,
        scratch_shapes=[
            vm((3, model), F32), vm((20, KP), BF16), vm((2, 10, KP), BF16),
            vm((SIDE, 4, UNIT, KP), BF16), vm((2, SIDE // 2, 2, 2, UNIT, KP), BF16),
            vm((4, 20, max(WIDTHS[0])), BF16), vm((8, 10, WMAX), BF16), vm((UNIT, WMAX), F32),
            dma((4,)), dma((4,)), dma((8,)), dma((8,)),
            dma((2, 7)), dma((2, 8)), dma((2, 2, 4, 8)), dma((2, 8, 8)), dma((3, 8)), dma((3, 8)), dma((2, 7, 8)),
            vm((n, KP), BF16), vm((n, HD), BF16), vm((n, HD), BF16), vm((band + 2, width, HD), F32),
            vm((n, HD), F32), vm((n, HD), BF16), vm((2, width, HD), BF16), vm((2, width, HD), BF16), vm((2, width, HD), BF16),
            vm((2, 192, 128), F32), vm((192, 128), F32), vm((SIDE, 24, 128), F32), vm((SIDE, 24, 128), F32),
            vm((24, 128), F32), vm((SIDE, 24, 128), F32), vm((24, 128), F32), vm((2, SIDE, 24, 128), F32),
            dma((2, 5)), dma((2, 5)), dma((2, 5)), dma((2, 5)), dma, dma, dma((8,)), dma((8,)), dma((8,)), dma((8,)), dma((8,)), dma((8,)), dma, dma,
        ],
        compiler_params=pltpu.CompilerParams(collective_id=0, has_side_effects=True, vmem_limit_bytes=50 << 20),
    )(
        tokens.reshape(n, model), shift, scale, gate, depth_taps,
        pair_weight.T, query_weight.T, output_weight,
    )
    return out.reshape(band, width, model), kvs


def solution(mesh):
    in_specs = (
        P(("clips", "rows"), None, None),
        P("clips"),
        P("clips"),
        P("clips"),
        P(None, "rows"),
        P(None, "rows"),
        P("rows", None),
        P(),
    )
    out_specs = (P(("clips", "rows"), None, None), P("clips", None, None))
    return jax.shard_map(body, mesh=mesh, in_specs=in_specs, out_specs=out_specs, check_vma=False)
```
